32 devices in a mesh: outer: 4 (over x, core), chip: 8 (over z, y).
Axes of the slice: x: 2, y: 2, z: 4, core: 2. Of those that a mesh axis runs over, the one named last changes fastest.
Arguments:
- inputs: bfloat16 [4096, 2048], P(('outer', 'chip')), may hold values from -6 to 6
- out_grads: bfloat16 [4096, 2048], P(('outer', 'chip')), may hold values from -6 to 6
- weight: bfloat16 [2048, 2048], P('chip'), may hold values from -0.125 to 0.125
- start_basis: float32 [64, 2048], P('chip'), may hold values from -6 to 6
- error_buffer: float32 [4, 2048, 2048], P('outer', 'chip'), may hold values from -2 to 2
Outputs:
- outputs: bfloat16 [4096, 2048], P(('outer', 'chip'))
- new_error: float32 [4, 2048, 2048], P('outer', 'chip')
The draws below stay inside these ranges and needn't reach their ends.
All inputs are finite; a program needn't handle non-finite values.
Results may differ from the reference program's by a relative error of at most 0.0085.
Values may be sent and summed in bfloat16 or wider, within the bound.
A program may use at most 128 MiB of HBM per device.

```python
import jax
import jax.numpy as jnp
from jax import lax

D = 2048
INNER = 2048
RANK = 8
TOK_DEV = 128
PODS = 4
QROWS = 64
TOKENS = 4096
N_CHIP = 8


def block_levels(own_key, extent, shards, least, high):
    def one(position, parts):
        draws = jax.random.uniform(jax.random.fold_in(jax.random.fold_in(own_key, 6), position), (parts,), jnp.float32, least / len(shards), high / len(shards))
        return jnp.repeat(jnp.exp(draws), extent[position] // parts).reshape((-1,) + (1,) * (len(extent) - position - 1))

    factor_of = one(*shards[0])
    for cut in shards[1:]:
        factor_of = factor_of * one(*cut)
    return factor_of


def centred(key, extent, scale, reach, shards=(), kind=jnp.bfloat16):
    level = block_levels(key, extent, shards, -0.22, 0.18) if shards else 1.0
    array = jax.random.normal(key, extent, jnp.float32) * scale * level
    return jnp.minimum(jnp.maximum(array, -reach), reach).astype(kind)


def setup_inputs(seed: int = 0) -> dict:
    keys = jax.random.split(jax.random.key(seed), 6)
    return {
        "inputs": centred(keys[0], (TOKENS, D), 1.0, 6.0, ((0, 32),)),
        "out_grads": centred(keys[1], (TOKENS, INNER), 1.0, 6.0, ((0, 32),)),
        "weight": centred(keys[2], (D, INNER), D ** -0.5, 0.125, ((0, 8),)),
        "start_basis": centred(keys[3], (QROWS, INNER), 1.0, 6.0, ((0, 8),), jnp.float32),
        "error_buffer": centred(keys[4], (PODS, D, INNER), 0.25, 2.0, ((0, 4), (1, 8)), jnp.float32),
    }


LEARNING_RATE = 0.2

def orthonormal(projected):
    finished = []
    for index in range(projected.shape[-2]):
        vector = projected[..., index, :]
        for unit in finished:
            vector = vector - lax.optimization_barrier(jnp.sum(vector * unit, axis=-1, keepdims=True)) * unit
        finished.append(vector / jnp.sqrt(lax.optimization_barrier(jnp.sum(vector * vector, axis=-1, keepdims=True)) + 1.0))
    return jnp.stack(finished, axis=-2)

def reference(inputs, out_grads, weight, start_basis, error_buffer):
    highest = lax.Precision.HIGHEST
    shard_rows = D // N_CHIP
    pod_tokens = TOK_DEV * N_CHIP
    basis_in = start_basis.reshape(N_CHIP, RANK, INNER)
    merged_all = []
    left_sum = jnp.zeros((N_CHIP, RANK, shard_rows), jnp.float32)
    for pod in range(PODS):
        pod_inputs = inputs[pod * pod_tokens:(pod + 1) * pod_tokens]
        pod_grads = out_grads[pod * pod_tokens:(pod + 1) * pod_tokens]
        gradient = lax.dot_general(pod_inputs, pod_grads, (((0,), (0,)), ((), ())), preferred_element_type=jnp.float32) / TOK_DEV
        merged = (gradient + error_buffer[pod]).reshape(N_CHIP, shard_rows, INNER)
        merged_all.append(merged)
        left_sum = left_sum + jnp.einsum('cki,cri->ckr', basis_in, merged, precision=highest)
    left_basis = orthonormal(left_sum / PODS)
    right_sum = jnp.zeros((N_CHIP, RANK, INNER), jnp.float32)
    for merged in merged_all:
        right_sum = right_sum + jnp.einsum('ckr,cri->cki', left_basis, merged, precision=highest)
    right_factor = right_sum / PODS
    approx = jnp.einsum('ckr,cki->cri', left_basis, right_factor, precision=highest)
    new_error = jnp.stack([merged - approx for merged in merged_all]).reshape(PODS, D, INNER)
    new_weight = (weight.astype(jnp.float32) - LEARNING_RATE * approx.reshape(D, INNER)).astype(jnp.bfloat16)
    outputs = jnp.dot(inputs, new_weight, preferred_element_type=jnp.float32).astype(jnp.bfloat16)
    return (outputs, new_error)
```

```python
import functools

import jax
import jax.numpy as jnp
from jax import lax
from jax.experimental import pallas as pl
from jax.experimental.pallas import tpu as pltpu
from jax.sharding import PartitionSpec as P

TOK_DEV = 128
LEARNING_RATE = 0.2
CHUNKS = 4
HELD = 2
F32 = jnp.float32
BF16 = jnp.bfloat16


def dot(a, b, ca, cb):
    return lax.dot_general(
        a, b, (((ca,), (cb,)), ((), ())), preferred_element_type=F32
    )


def halves(v):
    high = v.astype(BF16).astype(F32)
    return high, v - high


def stack(*parts):
    return jnp.concatenate(parts, axis=0).astype(BF16)


def split(thin):
    return stack(*halves(thin))


def fold(both):
    n = both.shape[0] // 2
    return both[:n] + both[n:]


def thin_dot(thin, wide_high, wide_low, cb):
    n = thin.shape[0]
    both = split(thin)
    return fold(dot(both, wide_high, 1, cb)) + dot(both[:n], wide_low, 1, cb)


def orthonormal(v):
    count = v.shape[0]
    row = lax.broadcasted_iota(jnp.int32, (count, 1), 0)
    for k in range(count):
        pivot = v[k : k + 1, :]
        d = jnp.sum(v * pivot, axis=1, keepdims=True)
        norm = d[k : k + 1, :] + 1.0
        scale = jnp.where(row > k, d / norm, 0.0)
        unit = pivot / jnp.sqrt(norm)
        v = jnp.where(row == k, unit, v - scale * pivot)
    return v


def kernel(
    A, B, PODS,
    x_hbm, g_hbm, w_hbm, basis_hbm, err_hbm,
    out_ref, ne_ref,
    xv, xg, xt, gg, wq, bas, ev, eh, el, ysend, yrecv, up_s, up_r, dn_s, dn_r,
    left_s, left_r, zs, zr, rp, rq, rz, rown, rall, own,
    in_sem, xs_sem, xr_sem, ws_sem, wr_sem, bs_sem, br_sem, gs_sem, gr_sem, ys_sem, yr_sem,
    rs_sem, rr_sem, ls_sem, lr_sem, zs_sem, zr_sem, hs_sem, hr_sem, ps_sem, pr_sem,
    as_sem, ar_sem, fs_sem, fr_sem,
):
    o = lax.axis_index("outer")
    c = lax.axis_index("chip")
    a, b = c // B, c % B
    T = x_hbm.shape[0]
    S, N = w_hbm.shape
    Q = B * S
    R = basis_hbm.shape[0]
    K = CHUNKS
    CN = N // K
    NP = N // PODS
    cols = [pl.ds(k * CN, CN) for k in range(K)]

    def rows_of(s):
        return pl.ds(pl.multiple_of(s * T, T), T)

    def shard_of(s):
        return pl.ds(pl.multiple_of(s * S, S), S)

    def share_of(s):
        return pl.ds(pl.multiple_of(s * NP, NP), NP)

    ins = [
        pltpu.make_async_copy(src, dst, in_sem.at[i])
        for i, (src, dst) in enumerate([
            (x_hbm, xv),
            (basis_hbm, bas.at[0]),
            (w_hbm, wq.at[shard_of(b)]),
            (g_hbm, gg.at[rows_of(a)]),
            (x_hbm.at[:, pl.ds(pl.multiple_of(a * Q, Q), Q)], xg.at[rows_of(a)]),
            (err_hbm, ev),
        ])
    ]
    for cp in ins:
        cp.start()

    line = [((a + d) % A) * B + b for d in range(1, A)]
    group = [(do, db) for do in range(PODS) for db in range(B) if do or db]

    def member(do, db):
        return {"outer": (o + do) % PODS, "chip": a * B + (b + db) % B}

    def remote(src, dst, ss, rs, where):
        return pltpu.make_async_remote_copy(
            src_ref=src, dst_ref=dst, send_sem=ss, recv_sem=rs,
            device_id=where, device_id_type=pl.DeviceIdType.MESH,
        )

    barrier = pltpu.get_barrier_semaphore()
    for t in line:
        pl.semaphore_signal(
            barrier, inc=1, device_id={"chip": t}, device_id_type=pl.DeviceIdType.MESH
        )
    for do, db in group:
        pl.semaphore_signal(
            barrier, inc=1, device_id=member(do, db), device_id_type=pl.DeviceIdType.MESH
        )
    pl.semaphore_wait(barrier, len(line) + len(group))

    x_copies = []
    for d in range(1, A):
        t = (a + d) % A
        x_copies.append(remote(
            xv.at[:, pl.ds(pl.multiple_of(t * Q, Q), Q)], xg.at[rows_of(a)],
            xs_sem.at[d], xr_sem.at[d], {"chip": t * B + b},
        ))
    b_copies = [
        remote(bas.at[0], bas.at[(-d) % B], bs_sem.at[d], br_sem.at[d], member(0, d))
        for d in range(1, B)
    ]

    def g_copy(direction, h, k):
        step = 1 if direction == 0 else -1
        source = a - step * (h - 1)
        place = gg.at[rows_of(source), cols[k]]
        return remote(
            place, place, gs_sem.at[direction, h, k], gr_sem.at[direction, h, k],
            {"chip": c + step * B},
        )

    def g_sends(direction, h):
        return (
            jnp.logical_and(a - (h - 1) >= 0, a + 1 < A)
            if direction == 0
            else jnp.logical_and(a + (h - 1) < A, a >= 1)
        )

    def g_gets(direction, h):
        return a - h >= 0 if direction == 0 else a + h < A

    def g_arrival(direction, h, k):
        step = 1 if direction == 0 else -1
        place = gg.at[rows_of(a - step * h), cols[k]]
        return remote(
            place, place, gs_sem.at[direction, h, k], gr_sem.at[direction, h, k],
            {"chip": c - step * B},
        )

    shared = PODS % 2 == 0
    mate = o + 1 - 2 * (o % 2)
    if shared:
        half = pl.ds(pl.multiple_of((o % 2) * (N // 2), N // 2), N // 2)
    else:
        half = pl.ds(0, N)
    w_copies, m_copies = [], []
    for d in range(1, B):
        w_copies.append(remote(
            wq.at[shard_of(b), half], wq.at[shard_of(b), half],
            ws_sem.at[0, d], wr_sem.at[0, d], member(0, d),
        ))
        if shared:
            came = (b - d + B) % B
            m_copies.append(remote(
                wq.at[shard_of(came), half], wq.at[shard_of(came), half],
                ws_sem.at[1, d], wr_sem.at[1, d], {"outer": mate},
            ))

    ins[0].wait()
    for cp in x_copies:
        cp.start()
    ins[1].wait()
    for cp in b_copies:
        cp.start()
    ins[2].wait()
    for cp in w_copies:
        cp.start()
    ins[3].wait()
    for k in range(K):
        for direction in range(2):
            @pl.when(g_sends(direction, 1))
            def _():
                g_copy(direction, 1, k).start()
    ins[4].wait()
    ins[5].wait()

    for k in range(K):
        high, low = halves(ev[:, cols[k]])
        eh[:, cols[k]] = high.astype(BF16)
        el[:, cols[k]] = low.astype(BF16)
    fed = thin_dot(bas[0], eh[...], el[...], 1)

    for cp in x_copies:
        cp.wait_recv()
    xt[...] = xg[...].T
    for cp in b_copies:
        cp.wait_recv()
    for cp in w_copies:
        cp.wait_recv()
    for cp in m_copies:
        cp.start()

    def y_copy(d, k):
        return remote(
            ysend.at[d - 1, :, cols[k]], yrecv.at[d - 1, :, cols[k]],
            ys_sem.at[d, k], yr_sem.at[d, k], member(0, d),
        )

    def gradient_chunk(k):
        for d in range(1, B):
            part = dot(xt[shard_of((b + d) % B), :], gg[:, cols[k]], 1, 0)
            ysend[d - 1, :, cols[k]] = part.astype(BF16)
            y_copy(d, k).start()
        ne_ref[:, cols[k]] = dot(xt[shard_of(b), :], gg[:, cols[k]], 1, 0)

    def merge_chunk(k):
        part = ne_ref[:, cols[k]]
        for d in range(1, B):
            y_copy(d, k).wait_recv()
            part = part + yrecv[d - 1, :, cols[k]].astype(F32)
        ne_ref[:, cols[k]] = part / TOK_DEV + ev[:, cols[k]]

    def project_chunk(k):
        basis = split(jnp.concatenate([bas[d, :, cols[k]] for d in range(B)], axis=0))
        return fold(dot(basis, gg[:, cols[k]], 1, 1))

    def o_copy(direction, r, k):
        s_buf, r_buf = (up_s, up_r) if direction == 0 else (dn_s, dn_r)
        return remote(
            s_buf.at[r - 1, :, cols[k]], r_buf.at[r - 1, :, cols[k]],
            rs_sem.at[direction, r, k], rr_sem.at[direction, r, k],
            {"chip": c + B if direction == 0 else c - B},
        )

    def o_first(direction):
        return a == 0 if direction == 0 else a == A - 1

    def o_sends(direction, r):
        return a + r < A if direction == 0 else a - r >= 0

    def o_gets(direction, r):
        if direction == 0:
            return jnp.logical_and(a >= 1, a - 1 + r < A)
        return jnp.logical_and(a + 1 < A, a + 1 - r >= 0)

    def out_piece(direction, r, k, first):
        s_buf, r_buf = (up_s, up_r) if direction == 0 else (dn_s, dn_r)
        leads = o_first(direction)
        if not first:
            leads = jnp.logical_not(leads)

        @pl.when(jnp.logical_and(o_sends(direction, r), leads))
        def _():
            token = a + r if direction == 0 else a - r
            part = dot(xg[rows_of(token), :], wq[:, cols[k]], 1, 0)
            if not first:
                o_copy(direction, r + 1, k).wait_recv()
                part = part + r_buf[r, :, cols[k]].astype(F32)
            s_buf[r - 1, :, cols[k]] = part.astype(BF16)
            o_copy(direction, r, k).start()

    def out_pieces(r, ks, first):
        for k in ks:
            for direction in range(2):
                out_piece(direction, r, k, first)

    early, held = range(K - HELD), range(K - HELD, K)
    l_copies = [
        remote(left_s, left_r.at[j], ls_sem.at[j], lr_sem.at[j], member(do, db))
        for j, (do, db) in enumerate(group)
    ]
    thin = jnp.zeros((B * R, A * T), F32)
    last = A - 2 + K
    for wave in range(1, last + 1):
        for h in range(1, A):
            k = wave - h
            if 0 <= k < K:
                for direction in range(2):
                    @pl.when(g_gets(direction, h))
                    def _():
                        g_arrival(direction, h, k).wait_recv()
                    if h + 1 < A:
                        @pl.when(g_sends(direction, h + 1))
                        def _():
                            g_copy(direction, h + 1, k).start()
        if wave == 1:
            for cp in m_copies:
                cp.wait_recv()
            for r in range(A - 1, 1, -1):
                out_pieces(r, range(K), True)
            out_pieces(1, early, True)
            for k in range(K):
                own[:, cols[k]] = dot(xg[rows_of(a), :], wq[:, cols[k]], 1, 0)
        k = wave - (A - 1)
        if 0 <= k < K:
            thin = thin + project_chunk(k)
            if k == K - 1:
                for d in range(B):
                    mine = thin[d * R : (d + 1) * R, :]
                    part = fold(dot(split(mine), xg[:, shard_of((b + d) % B)], 1, 0)) / TOK_DEV
                    left_s[d] = part + fed if d == 0 else part
                for cp in l_copies:
                    cp.start()
            gradient_chunk(k)
            if k >= 1:
                merge_chunk(k - 1)
    for r in range(A - 2, 1, -1):
        out_pieces(r, range(K), False)

    total = [left_s[d] for d in range(B)]
    for j, (do, db) in enumerate(group):
        l_copies[j].wait_recv()
        for d in range(B):
            total[d] = total[d] + left_r[j, (d + db) % B]
    left = [orthonormal(total[d] / PODS) for d in range(B)]

    z = jnp.concatenate(
        [fold(dot(split(left[d]), xt[shard_of((b + d) % B), :], 1, 0)) for d in range(B)], axis=0
    )
    for t in range(A):
        zs[t] = z[:, t * T : (t + 1) * T]
    z_copies = []
    for d in range(1, A):
        t = (a + d) % A
        z_copies.append(remote(
            zs.at[t], zr.at[a], zs_sem.at[d], zr_sem.at[d], {"chip": t * B + b}
        ))
    z_pair = split(z)
    for k in range(K):
        part = fold(dot(z_pair, gg[:, cols[k]], 1, 0)) / TOK_DEV
        lead = part[:R] + thin_dot(left[0], eh[:, cols[k]], el[:, cols[k]], 0)
        rp[0, :, cols[k]] = lead.astype(BF16)
        for d in range(1, B):
            rp[d, :, cols[k]] = part[d * R : (d + 1) * R].astype(BF16)
    h_copies = [
        remote(
            rp.at[db, :, share_of((o + do) % PODS)], rq.at[j],
            hs_sem.at[j], hr_sem.at[j], member(do, db),
        )
        for j, (do, db) in enumerate(group)
    ]
    for cp in h_copies:
        cp.start()
    for cp in z_copies:
        cp.start()
    zr[a] = zs[a]
    out_pieces(1, early, False)

    right = rp[0, :, share_of(o)].astype(F32)
    for j, cp in enumerate(h_copies):
        cp.wait_recv()
        right = right + rq[j].astype(F32)
    rz[a] = (right / PODS).astype(BF16)
    p_copies = [
        remote(
            rz.at[a], rown.at[:, share_of(o)], ps_sem.at[do], pr_sem.at[do], member(do, 0)
        )
        for do in range(1, PODS)
    ]
    a_copies = [
        remote(rz.at[a], rz.at[a], as_sem.at[d + 1], ar_sem.at[d + 1], {"chip": t})
        for d, t in enumerate(line)
    ]
    for cp in a_copies + p_copies:
        cp.start()
    rown[:, share_of(o)] = rz[a]
    for first in (True, False):
        out_pieces(1, held, first)
    merge_chunk(K - 1)

    for cp in a_copies:
        cp.wait_recv()
    f_copies = [
        remote(
            rz, rall.at[(-db) % B, :, :, share_of(o)], fs_sem.at[j], fr_sem.at[j], member(do, db)
        )
        for j, (do, db) in enumerate(group)
    ]
    for cp in f_copies:
        cp.start()
    rall[0, :, :, share_of(o)] = rz[...]
    for cp in p_copies:
        cp.wait_recv()
    lefts = split(left[0])
    for k in range(K):
        mine = rown[:, cols[k]].astype(F32)
        ne_ref[:, cols[k]] = ne_ref[:, cols[k]] - dot(lefts, stack(mine, mine), 0, 0)

    for cp in z_copies:
        cp.wait_recv()
    z = split(jnp.concatenate(
        [zr[t, d * R : (d + 1) * R, :] for d in range(B) for t in range(A)], axis=0
    ))
    for cp in f_copies:
        cp.wait_recv()
    for k in range(K):
        rights = jnp.concatenate(
            [rall[d, t, :, cols[k]].astype(F32) for d in range(B) for t in range(A)], axis=0
        )
        delta = dot(z, stack(rights, rights), 0, 0)
        for direction in range(2):
            r_buf = up_r if direction == 0 else dn_r

            @pl.when(o_gets(direction, 1))
            def _():
                o_copy(direction, 1, k).wait_recv()

            @pl.when(jnp.logical_not(o_gets(direction, 1)))
            def _():
                r_buf[0, :, cols[k]] = jnp.zeros((T, CN), BF16)
        mine = own[:, cols[k]] + up_r[0, :, cols[k]].astype(F32) + dn_r[0, :, cols[k]].astype(F32)
        out_ref[:, cols[k]] = (mine - LEARNING_RATE * delta).astype(BF16)

    for cp in x_copies + b_copies + w_copies + m_copies + l_copies + z_copies + h_copies:
        cp.wait_send()
    for cp in p_copies + a_copies + f_copies:
        cp.wait_send()
    for k in range(K):
        for d in range(1, B):
            y_copy(d, k).wait_send()
        for direction in range(2):
            for h in range(1, A):
                @pl.when(g_sends(direction, h))
                def _():
                    g_copy(direction, h, k).wait_send()

                @pl.when(o_sends(direction, h))
                def _():
                    o_copy(direction, h, k).wait_send()


def shards(inputs, out_grads, weight, start_basis, error_buffer):
    PODS, NC = lax.axis_size("outer"), lax.axis_size("chip")
    A = 4 if NC % 4 == 0 else NC
    B = NC // A
    T, D = inputs.shape
    N = out_grads.shape[1]
    S = weight.shape[0]
    R = start_basis.shape[0]
    Q = B * S
    K = CHUNKS
    G = PODS * B
    dma = pltpu.SemaphoreType.DMA
    vmem = pl.BlockSpec(memory_space=pltpu.VMEM)
    hbm = pl.BlockSpec(memory_space=pltpu.HBM)
    outputs, new_error = pl.pallas_call(
        functools.partial(kernel, A, B, PODS),
        out_shape=(
            jax.ShapeDtypeStruct((T, N), BF16),
            jax.ShapeDtypeStruct((S, N), F32),
        ),
        in_specs=[hbm] * 5,
        out_specs=(vmem, vmem),
        scratch_shapes=[
            pltpu.VMEM((T, D), BF16),
            pltpu.VMEM((A * T, Q), BF16),
            pltpu.VMEM((Q, A * T), BF16),
            pltpu.VMEM((A * T, N), BF16),
            pltpu.VMEM((Q, N), BF16),
            pltpu.VMEM((B, R, N), F32),
            pltpu.VMEM((S, N), F32),
            pltpu.VMEM((S, N), BF16),
            pltpu.VMEM((S, N), BF16),
            pltpu.VMEM((B - 1, S, N), BF16),
            pltpu.VMEM((B - 1, S, N), BF16),
            pltpu.VMEM((A - 1, T, N), BF16),
            pltpu.VMEM((A - 1, T, N), BF16),
            pltpu.VMEM((A - 1, T, N), BF16),
            pltpu.VMEM((A - 1, T, N), BF16),
            pltpu.VMEM((B, R, S), F32),
            pltpu.VMEM((G - 1, B, R, S), F32),
            pltpu.VMEM((A, B * R, T), F32),
            pltpu.VMEM((A, B * R, T), F32),
            pltpu.VMEM((B, R, N), BF16),
            pltpu.VMEM((G - 1, R, N // PODS), BF16),
            pltpu.VMEM((A, R, N // PODS), BF16),
            pltpu.VMEM((R, N), BF16),
            pltpu.VMEM((B, A, R, N), BF16),
            pltpu.VMEM((T, N), F32),
            dma((6,)), dma((A,)), dma((A,)), dma((2, B)), dma((2, B)), dma((B,)), dma((B,)),
            dma((2, A, K)), dma((2, A, K)), dma((B, K)), dma((B, K)),
            dma((2, A, K)), dma((2, A, K)),
            dma((G,)), dma((G,)), dma((A,)), dma((A,)), dma((G,)), dma((G,)),
            dma((PODS,)), dma((PODS,)), dma((A,)), dma((A,)), dma((G,)), dma((G,)),
        ],
        compiler_params=pltpu.CompilerParams(
            collective_id=0, has_side_effects=True, vmem_limit_bytes=40 * 1024 * 1024
        ),
        name="step",
    )(inputs, out_grads, weight, start_basis, error_buffer[0])
    return outputs, new_error[None]


def solution(mesh):
    return jax.shard_map(
        shards,
        mesh=mesh,
        in_specs=(
            P(("outer", "chip"), None),
            P(("outer", "chip"), None),
            P("chip", None),
            P("chip", None),
            P("outer", "chip", None),
        ),
        out_specs=(P(("outer", "chip"), None), P("outer", "chip", None)),
        check_vma=False,
    )
```

```python
import functools

import jax
import jax.numpy as jnp
from jax import lax
from jax.experimental import pallas as pl
from jax.experimental.pallas import tpu as pltpu
from jax.sharding import PartitionSpec as P

TOK_DEV = 128
LEARNING_RATE = 0.2
CHUNKS = 8
AHEAD = 4
PIECES = 2
F32 = jnp.float32
BF16 = jnp.bfloat16


def dot(a, b, ca, cb):
    return lax.dot_general(
        a, b, (((ca,), (cb,)), ((), ())), preferred_element_type=F32
    )


def halves(v):
    high = v.astype(BF16).astype(F32)
    return high, v - high


def stack(*parts):
    return jnp.concatenate(parts, axis=0).astype(BF16)


def split(thin):
    return stack(*halves(thin))


def fold(both):
    n = both.shape[0] // 2
    return both[:n] + both[n:]


def thin_dot(thin, wide_high, wide_low, cb):
    n = thin.shape[0]
    both = split(thin)
    return fold(dot(both, wide_high, 1, cb)) + dot(both[:n], wide_low, 1, cb)


def orthonormal(v):
    count = v.shape[0]
    row = lax.broadcasted_iota(jnp.int32, (count, 1), 0)
    for k in range(count):
        pivot = v[k : k + 1, :]
        d = jnp.sum(v * pivot, axis=1, keepdims=True)
        norm = d[k : k + 1, :] + 1.0
        scale = jnp.where(row > k, d / norm, 0.0)
        unit = pivot / jnp.sqrt(norm)
        v = jnp.where(row == k, unit, v - scale * pivot)
    return v


def plan_of(A, K):
    firsts = [("first", r, k) for r in range(A - 1, 0, -1) for k in range(K)]
    rests = [("rest", r, k) for r in range(A - 2, 0, -1) for k in range(K)]

    def take(queue, count):
        taken = queue[:count]
        del queue[:count]
        return taken

    last = A - 2 + K
    chain = {
        2: ["weights", "mates"], 3: ["left1"], 5: ["left2", "own"], last - 3: ["right1"],
        last - 2: ["right2"], last - 1: ["right3"],
    }
    steps = []
    for wave in range(1, last + 1):
        steps.append(("wave", wave))
        if wave == last - 2:
            steps += take(rests, 3)
        steps += [(name,) for name in chain.get(wave, [])]
        if wave >= 3:
            steps += take(firsts, A - 1)
        if wave >= last - 3:
            steps += take(rests, 3)
    steps += [("right4",)] + firsts + rests
    return steps + [("merge", k) for k in range(K)]


def kernel(
    A, B, PODS,
    x_hbm, g_hbm, w_hbm, basis_hbm, err_hbm,
    out_ref, ne_ref,
    xv, xg, xt, gg, wq, bas, bz, ball, ev, eh, el, ysend, yrecv, up_s, up_r, dn_s, dn_r,
    ls, lz, left_s, left_r, zs, zr, rp, rq, rs, rw, rz, rown, rall, own,
    in_sem, xs_sem, xr_sem, ws_sem, wr_sem, cs_sem, cr_sem, vs_sem, vr_sem, bs_sem, br_sem,
    gs_sem, gr_sem, ys_sem, yr_sem, rs_sem, rr_sem, js_sem, jr_sem, ls_sem, lr_sem, zs_sem, zr_sem,
    hs_sem, hr_sem, ts_sem, tr_sem, ps_sem, pr_sem, as_sem, ar_sem, fs_sem, fr_sem,
):
    o = lax.axis_index("outer")
    c = lax.axis_index("chip")
    a, b = c // B, c % B
    T = x_hbm.shape[0]
    S, N = w_hbm.shape
    Q = B * S
    R = basis_hbm.shape[0]
    K = CHUNKS
    CN = N // K
    NP = N // PODS
    cols = [pl.ds(k * CN, CN) for k in range(K)]

    def rows_of(s):
        return pl.ds(pl.multiple_of(s * T, T), T)

    def shard_of(s):
        return pl.ds(pl.multiple_of(s * S, S), S)

    def share_of(s):
        return pl.ds(pl.multiple_of(s * NP, NP), NP)

    ins = [
        pltpu.make_async_copy(src, dst, in_sem.at[i])
        for i, (src, dst) in enumerate([
            (basis_hbm.at[:, share_of(o)], bz.at[a]),
            (x_hbm, xv),
            (g_hbm, gg.at[rows_of(a)]),
            (w_hbm, wq.at[shard_of(b)]),
            (basis_hbm, bas),
            (x_hbm.at[:, pl.ds(pl.multiple_of(a * Q, Q), Q)], xg.at[rows_of(a)]),
            (err_hbm, ev),
        ])
    ]
    for cp in ins:
        cp.start()

    line = [((a + d) % A) * B + b for d in range(1, A)]
    group = [(do, db) for do in range(PODS) for db in range(B) if do or db]

    def member(do, db):
        return {"outer": (o + do) % PODS, "chip": a * B + (b + db) % B}

    def remote(src, dst, ss, rs, where):
        return pltpu.make_async_remote_copy(
            src_ref=src, dst_ref=dst, send_sem=ss, recv_sem=rs,
            device_id=where, device_id_type=pl.DeviceIdType.MESH,
        )

    barrier = pltpu.get_barrier_semaphore()
    for t in line:
        pl.semaphore_signal(
            barrier, inc=1, device_id={"chip": t}, device_id_type=pl.DeviceIdType.MESH
        )
    for do, db in group:
        pl.semaphore_signal(
            barrier, inc=1, device_id=member(do, db), device_id_type=pl.DeviceIdType.MESH
        )
    pl.semaphore_wait(barrier, len(line) + len(group))

    x_copies = []
    for d in range(1, A):
        t = (a + d) % A
        x_copies.append(remote(
            xv.at[:, pl.ds(pl.multiple_of(t * Q, Q), Q)], xg.at[rows_of(a)],
            xs_sem.at[d], xr_sem.at[d], {"chip": t * B + b},
        ))
    def along(src, dst, ss, rs):
        return [
            remote(src((a + d) % A), dst, ss.at[d], rs.at[d], {"chip": ((a + d) % A) * B + b})
            for d in range(1, A)
        ]

    def across(src, dst, ss, rs):
        return [
            remote(src(do, db), dst(j, db), ss.at[j], rs.at[j], member(do, db))
            for j, (do, db) in enumerate(group)
        ]

    c_copies = along(lambda t: bz.at[a], bz.at[a], cs_sem, cr_sem)
    b_copies = [
        [
            remote(
                bz if d == 0 else ball.at[d, :, :, share_of(o)],
                ball.at[d, :, :, share_of(o)],
                bs_sem.at[d, do], br_sem.at[d, do], member(do, 0),
            )
            for do in range(1, PODS)
        ]
        for d in range(B)
    ]
    v_copies = [
        remote(bz, ball.at[(-d) % B, :, :, share_of(o)], vs_sem.at[d], vr_sem.at[d], member(0, d))
        for d in range(1, B)
    ]

    def g_copy(direction, h, k):
        step = 1 if direction == 0 else -1
        source = a - step * (h - 1)
        place = gg.at[rows_of(source), cols[k]]
        return remote(
            place, place, gs_sem.at[direction, h, k], gr_sem.at[direction, h, k],
            {"chip": c + step * B},
        )

    def g_sends(direction, h):
        return (
            jnp.logical_and(a - (h - 1) >= 0, a + 1 < A)
            if direction == 0
            else jnp.logical_and(a + (h - 1) < A, a >= 1)
        )

    def g_gets(direction, h):
        return a - h >= 0 if direction == 0 else a + h < A

    def g_arrival(direction, h, k):
        step = 1 if direction == 0 else -1
        place = gg.at[rows_of(a - step * h), cols[k]]
        return remote(
            place, place, gs_sem.at[direction, h, k], gr_sem.at[direction, h, k],
            {"chip": c - step * B},
        )

    shared = PODS % 2 == 0
    mate = o + 1 - 2 * (o % 2)
    base, WN = (o % 2 * (N // 2), N // 2 // PIECES) if shared else (0, N // PIECES)
    w_copies, m_copies = [[] for _ in range(PIECES)], [[] for _ in range(PIECES)]
    for i in range(PIECES):
        piece = pl.ds(pl.multiple_of(base + i * WN, WN), WN)
        for d in range(1, B):
            here = wq.at[shard_of(b), piece]
            w_copies[i].append(
                remote(here, here, ws_sem.at[0, i, d], wr_sem.at[0, i, d], member(0, d))
            )
            if shared:
                came = wq.at[shard_of((b - d + B) % B), piece]
                m_copies[i].append(
                    remote(came, came, ws_sem.at[1, i, d], wr_sem.at[1, i, d], {"outer": mate})
                )

    def g_first(k):
        for direction in range(2):
            @pl.when(g_sends(direction, 1))
            def _():
                g_copy(direction, 1, k).start()

    ins[0].wait()
    for cp in c_copies:
        cp.start()
    ins[1].wait()
    for cp in x_copies:
        cp.start()
    ins[2].wait()
    for k in range(AHEAD):
        g_first(k)
    ins[3].wait()
    for cp in w_copies[0]:
        cp.start()
    for cp in ins[4:]:
        cp.wait()

    for k in range(K):
        high, low = halves(ev[:, cols[k]])
        eh[:, cols[k]] = high.astype(BF16)
        el[:, cols[k]] = low.astype(BF16)
    fed = thin_dot(bas[...], eh[...], el[...], 1)

    for cp in c_copies:
        cp.wait_recv()
    for cp in v_copies + b_copies[0]:
        cp.start()
    for copies in w_copies[1:]:
        for cp in copies:
            cp.start()
    ball[0, :, :, share_of(o)] = bz[...]
    for d in range(1, B):
        v_copies[B - d - 1].wait_recv()
        for cp in b_copies[d]:
            cp.start()
    for copies in b_copies:
        for cp in copies:
            cp.wait_recv()
    thin = jnp.zeros((B * A * R, T), F32)
    for k in range(K):
        basis = split(jnp.concatenate(
            [ball[d, t, :, cols[k]] for d in range(B) for t in range(A)], axis=0
        ))
        thin = thin + fold(dot(basis, gg[rows_of(a), cols[k]], 1, 1))
    for d in range(B):
        for t in range(A):
            row = (d * A + t) * R
            shard = shard_of(t * B + (b + d) % B)
            ls[t, d] = fold(dot(split(thin[row : row + R, :]), xv[:, shard], 1, 0)) / TOK_DEV
    j_copies = along(lambda t: ls.at[t], lz.at[a], js_sem, jr_sem)
    for cp in j_copies:
        cp.start()
    lz[a] = ls[a]

    for cp in x_copies:
        cp.wait_recv()
    xt[...] = xg[...].T

    def y_copy(d, k):
        return remote(
            ysend.at[d - 1, :, cols[k]], yrecv.at[d - 1, :, cols[k]],
            ys_sem.at[d, k], yr_sem.at[d, k], member(0, d),
        )

    def gradient_chunk(k):
        for d in range(1, B):
            part = dot(xt[shard_of((b + d) % B), :], gg[:, cols[k]], 1, 0)
            ysend[d - 1, :, cols[k]] = part.astype(BF16)
            y_copy(d, k).start()
        ne_ref[:, cols[k]] = dot(xt[shard_of(b), :], gg[:, cols[k]], 1, 0)

    def merge_chunk(k):
        part = ne_ref[:, cols[k]]
        for d in range(1, B):
            y_copy(d, k).wait_recv()
            part = part + yrecv[d - 1, :, cols[k]].astype(F32)
        ne_ref[:, cols[k]] = part / TOK_DEV + ev[:, cols[k]]

    def o_copy(direction, r, k):
        s_buf, r_buf = (up_s, up_r) if direction == 0 else (dn_s, dn_r)
        return remote(
            s_buf.at[r - 1, :, cols[k]], r_buf.at[r - 1, :, cols[k]],
            rs_sem.at[direction, r, k], rr_sem.at[direction, r, k],
            {"chip": c + B if direction == 0 else c - B},
        )

    def o_first(direction):
        return a == 0 if direction == 0 else a == A - 1

    def o_sends(direction, r):
        return a + r < A if direction == 0 else a - r >= 0

    def o_gets(direction, r):
        if direction == 0:
            return jnp.logical_and(a >= 1, a - 1 + r < A)
        return jnp.logical_and(a + 1 < A, a + 1 - r >= 0)

    def out_piece(direction, r, k, first):
        s_buf, r_buf = (up_s, up_r) if direction == 0 else (dn_s, dn_r)
        leads = o_first(direction)
        if not first:
            leads = jnp.logical_not(leads)

        @pl.when(jnp.logical_and(o_sends(direction, r), leads))
        def _():
            token = a + r if direction == 0 else a - r
            part = dot(xg[rows_of(token), :], wq[:, cols[k]], 1, 0)
            if not first:
                o_copy(direction, r + 1, k).wait_recv()
                part = part + r_buf[r, :, cols[k]].astype(F32)
            s_buf[r - 1, :, cols[k]] = part.astype(BF16)
            o_copy(direction, r, k).start()

    def weights_in():
        for came, passed in zip(w_copies, m_copies):
            for cp in came:
                cp.wait_recv()
            for cp in passed:
                cp.start()

    def mates_in():
        for copies in m_copies:
            for cp in copies:
                cp.wait_recv()

    def first_piece(r, k):
        for direction in range(2):
            out_piece(direction, r, k, True)

    def rest_piece(r, k):
        for direction in range(2):
            out_piece(direction, r, k, False)

    l_copies = across(lambda do, db: left_s, lambda j, db: left_r.at[j], ls_sem, lr_sem)
    z_copies = along(lambda t: zs.at[t], zr.at[a], zs_sem, zr_sem)
    h_copies = across(
        lambda do, db: rp.at[db, :, :, share_of((o + do) % PODS)],
        lambda j, db: rq.at[j], hs_sem, hr_sem,
    )
    t_copies = along(lambda t: rs.at[t], rw.at[a], ts_sem, tr_sem)
    a_copies = along(lambda t: rz.at[a], rz.at[a], as_sem, ar_sem)
    p_copies = [
        remote(
            rz.at[a], rown.at[:, share_of(o)], ps_sem.at[do], pr_sem.at[do], member(do, 0)
        )
        for do in range(1, PODS)
    ]
    f_copies = across(
        lambda do, db: rz, lambda j, db: rall.at[(-db) % B, :, :, share_of(o)], fs_sem, fr_sem
    )

    def left_line():
        for cp in j_copies:
            cp.wait_recv()
        for d in range(B):
            part = lz[0, d]
            for t in range(1, A):
                part = part + lz[t, d]
            left_s[d] = part + fed if d == 0 else part
        for cp in l_copies:
            cp.start()

    left = []

    def left_done():
        total = [left_s[d] for d in range(B)]
        for j, (do, db) in enumerate(group):
            l_copies[j].wait_recv()
            for d in range(B):
                total[d] = total[d] + left_r[j, (d + db) % B]
        left.extend(orthonormal(total[d] / PODS) for d in range(B))
        z = jnp.concatenate(
            [fold(dot(split(left[d]), xt[shard_of((b + d) % B), :], 1, 0)) for d in range(B)],
            axis=0,
        )
        for t in range(A):
            zs[t] = z[:, t * T : (t + 1) * T]
        for cp in z_copies:
            cp.start()
        zr[a] = zs[a]

    z_all = []

    def right_part():
        for cp in z_copies:
            cp.wait_recv()
        z_all.append(split(jnp.concatenate(
            [zr[t, d * R : (d + 1) * R, :] for d in range(B) for t in range(A)], axis=0
        )))
        for k in range(K):
            part = fold(dot(z_all[0], gg[rows_of(a), cols[k]], 1, 0)) / TOK_DEV
            lead = thin_dot(left[0], eh[:, cols[k]], el[:, cols[k]], 0)
            for d in range(B):
                for t in range(A):
                    row = (d * A + t) * R
                    piece = part[row : row + R]
                    if d == 0:
                        piece = piece + jnp.where(a == t, lead, 0.0)
                    rp[d, t, :, cols[k]] = piece.astype(BF16)
        for cp in h_copies:
            cp.start()

    def right_group():
        right = rp[0, :, :, share_of(o)].astype(F32)
        for j, cp in enumerate(h_copies):
            cp.wait_recv()
            right = right + rq[j].astype(F32)
        rs[...] = right.astype(BF16)
        for cp in t_copies:
            cp.start()
        rw[a] = rs[a]

    def right_line():
        for cp in t_copies:
            cp.wait_recv()
        right = rw[0].astype(F32)
        for t in range(1, A):
            right = right + rw[t].astype(F32)
        rz[a] = (right / PODS).astype(BF16)
        for cp in a_copies + p_copies:
            cp.start()
        rown[:, share_of(o)] = rz[a]

    def right_all():
        for cp in a_copies:
            cp.wait_recv()
        for cp in f_copies:
            cp.start()
        rall[0, :, :, share_of(o)] = rz[...]

    def own_out():
        for k in range(K):
            own[:, cols[k]] = dot(xg[rows_of(a), :], wq[:, cols[k]], 1, 0)

    def wave(step):
        for h in range(1, A):
            k = step - h
            if 0 <= k < K:
                for direction in range(2):
                    @pl.when(g_gets(direction, h))
                    def _():
                        g_arrival(direction, h, k).wait_recv()
                    if h + 1 < A:
                        @pl.when(g_sends(direction, h + 1))
                        def _():
                            g_copy(direction, h + 1, k).start()
        k = step - 1 + AHEAD
        if k < K:
            g_first(k)
        k = step - (A - 1)
        if 0 <= k < K:
            gradient_chunk(k)

    actions = {
        "wave": wave, "weights": weights_in, "mates": mates_in, "left1": left_line,
        "left2": left_done, "right1": right_part, "right2": right_group,
        "right3": right_line, "right4": right_all, "own": own_out,
        "first": first_piece, "rest": rest_piece, "merge": merge_chunk,
    }
    for kind, *args in plan_of(A, K):
        actions[kind](*args)

    for cp in p_copies:
        cp.wait_recv()
    lefts = split(left[0])
    for k in range(K):
        mine = rown[:, cols[k]].astype(F32)
        ne_ref[:, cols[k]] = ne_ref[:, cols[k]] - dot(lefts, stack(mine, mine), 0, 0)

    for cp in f_copies:
        cp.wait_recv()
    for k in range(K):
        rights = jnp.concatenate(
            [rall[d, t, :, cols[k]].astype(F32) for d in range(B) for t in range(A)], axis=0
        )
        delta = dot(z_all[0], stack(rights, rights), 0, 0)
        for direction in range(2):
            r_buf = up_r if direction == 0 else dn_r

            @pl.when(o_gets(direction, 1))
            def _():
                o_copy(direction, 1, k).wait_recv()

            @pl.when(jnp.logical_not(o_gets(direction, 1)))
            def _():
                r_buf[0, :, cols[k]] = jnp.zeros((T, CN), BF16)
        mine = own[:, cols[k]] + up_r[0, :, cols[k]].astype(F32) + dn_r[0, :, cols[k]].astype(F32)
        out_ref[:, cols[k]] = (mine - LEARNING_RATE * delta).astype(BF16)

    for copies in b_copies + w_copies + m_copies:
        for cp in copies:
            cp.wait_send()
    for cp in c_copies + v_copies + x_copies + j_copies + l_copies:
        cp.wait_send()
    for cp in z_copies + h_copies + t_copies + p_copies + a_copies + f_copies:
        cp.wait_send()
    for k in range(K):
        for d in range(1, B):
            y_copy(d, k).wait_send()
        for direction in range(2):
            for h in range(1, A):
                @pl.when(g_sends(direction, h))
                def _():
                    g_copy(direction, h, k).wait_send()

                @pl.when(o_sends(direction, h))
                def _():
                    o_copy(direction, h, k).wait_send()


def shards(inputs, out_grads, weight, start_basis, error_buffer):
    PODS, NC = lax.axis_size("outer"), lax.axis_size("chip")
    A = 4 if NC % 4 == 0 else NC
    B = NC // A
    T, D = inputs.shape
    N = out_grads.shape[1]
    S = weight.shape[0]
    R = start_basis.shape[0]
    Q = B * S
    K = CHUNKS
    G = PODS * B
    dma = pltpu.SemaphoreType.DMA
    vmem = pl.BlockSpec(memory_space=pltpu.VMEM)
    hbm = pl.BlockSpec(memory_space=pltpu.HBM)
    outputs, new_error = pl.pallas_call(
        functools.partial(kernel, A, B, PODS),
        out_shape=(
            jax.ShapeDtypeStruct((T, N), BF16),
            jax.ShapeDtypeStruct((S, N), F32),
        ),
        in_specs=[hbm] * 5,
        out_specs=(vmem, vmem),
        scratch_shapes=[
            pltpu.VMEM((T, D), BF16),
            pltpu.VMEM((A * T, Q), BF16),
            pltpu.VMEM((Q, A * T), BF16),
            pltpu.VMEM((A * T, N), BF16),
            pltpu.VMEM((Q, N), BF16),
            pltpu.VMEM((R, N), F32),
            pltpu.VMEM((A, R, N // PODS), F32),
            pltpu.VMEM((B, A, R, N), F32),
            pltpu.VMEM((S, N), F32),
            pltpu.VMEM((S, N), BF16),
            pltpu.VMEM((S, N), BF16),
            pltpu.VMEM((B - 1, S, N), BF16),
            pltpu.VMEM((B - 1, S, N), BF16),
            pltpu.VMEM((A - 1, T, N), BF16),
            pltpu.VMEM((A - 1, T, N), BF16),
            pltpu.VMEM((A - 1, T, N), BF16),
            pltpu.VMEM((A - 1, T, N), BF16),
            pltpu.VMEM((A, B, R, S), F32),
            pltpu.VMEM((A, B, R, S), F32),
            pltpu.VMEM((B, R, S), F32),
            pltpu.VMEM((G - 1, B, R, S), F32),
            pltpu.VMEM((A, B * R, T), F32),
            pltpu.VMEM((A, B * R, T), F32),
            pltpu.VMEM((B, A, R, N), BF16),
            pltpu.VMEM((G - 1, A, R, N // PODS), BF16),
            pltpu.VMEM((A, R, N // PODS), BF16),
            pltpu.VMEM((A, R, N // PODS), BF16),
            pltpu.VMEM((A, R, N // PODS), BF16),
            pltpu.VMEM((R, N), BF16),
            pltpu.VMEM((B, A, R, N), BF16),
            pltpu.VMEM((T, N), F32),
            dma((7,)), dma((A,)), dma((A,)), dma((2, PIECES, B)), dma((2, PIECES, B)),
            dma((A,)), dma((A,)), dma((B,)), dma((B,)), dma((B, PODS)), dma((B, PODS)),
            dma((2, A, K)), dma((2, A, K)),
            dma((B, K)), dma((B, K)), dma((2, A, K)), dma((2, A, K)),
            dma((A,)), dma((A,)), dma((G,)), dma((G,)), dma((A,)), dma((A,)),
            dma((G,)), dma((G,)), dma((A,)), dma((A,)),
            dma((PODS,)), dma((PODS,)), dma((A,)), dma((A,)), dma((G,)), dma((G,)),
        ],
        compiler_params=pltpu.CompilerParams(
            collective_id=0, has_side_effects=True, vmem_limit_bytes=40 * 1024 * 1024
        ),
        name="step",
    )(*[
        pltpu.with_memory_space_constraint(t, pltpu.HBM)
        for t in (inputs, out_grads, weight, start_basis, error_buffer[0])
    ])
    return outputs, new_error[None]


def solution(mesh):
    return jax.shard_map(
        shards,
        mesh=mesh,
        in_specs=(
            P(("outer", "chip"), None),
            P(("outer", "chip"), None),
            P("chip", None),
            P("chip", None),
            P("outer", "chip", None),
        ),
        out_specs=(P(("outer", "chip"), None), P("outer", "chip", None)),
        check_vma=False,
    )
```

```python
import functools

import jax
import jax.numpy as jnp
from jax import lax
from jax.experimental import pallas as pl
from jax.experimental.pallas import tpu as pltpu
from jax.sharding import PartitionSpec as P

TOK_DEV = 128
LEARNING_RATE = 0.2
CHUNKS = 8
AHEAD = 4
PIECES = 2
FAMILIES = "abcfhjlmptvxyzw"
F32 = jnp.float32
BF16 = jnp.bfloat16


def dot(a, b, ca, cb):
    return lax.dot_general(
        a, b, (((ca,), (cb,)), ((), ())), preferred_element_type=F32
    )


def halves(v):
    high = v.astype(BF16).astype(F32)
    return high, v - high


def stack(*parts):
    return jnp.concatenate(parts, axis=0).astype(BF16)


def split(thin):
    return stack(*halves(thin))


def fold(both):
    n = both.shape[0] // 2
    return both[:n] + both[n:]


def thin_dot(thin, wide_high, wide_low, cb):
    n = thin.shape[0]
    both = split(thin)
    return fold(dot(both, wide_high, 1, cb)) + dot(both[:n], wide_low, 1, cb)


def orthonormal(v):
    count = v.shape[0]
    row = lax.broadcasted_iota(jnp.int32, (count, 1), 0)
    for k in range(count):
        pivot = v[k : k + 1, :]
        d = jnp.sum(v * pivot, axis=1, keepdims=True)
        norm = d[k : k + 1, :] + 1.0
        scale = jnp.where(row > k, d / norm, 0.0)
        unit = pivot / jnp.sqrt(norm)
        v = jnp.where(row == k, unit, v - scale * pivot)
    return v


def plan_of(A, K):
    firsts = [("first", r, k) for r in range(A - 1, 0, -1) for k in range(K)]
    rests = [("rest", r, k) for r in range(A - 2, 0, -1) for k in range(K)]

    def take(queue, count):
        taken = queue[:count]
        del queue[:count]
        return taken

    last = A - 2 + K
    chain = {
        1: ["basis"], 2: ["left0", "x", "weights", "mates"], 3: ["left1"], 5: ["left2", "own"], last - 3: ["right1"],
        last - 2: ["right2"], last - 1: ["right3"],
    }
    steps = []
    for wave in range(1, last + 1):
        steps.append(("wave", wave))
        if wave == last - 2:
            steps += take(rests, 3)
        steps += [(name,) for name in chain.get(wave, [])]
        if wave >= 3:
            steps += take(firsts, A - 1)
        if wave >= last - 3:
            steps += take(rests, 3)
    steps += [("right4",)] + firsts + rests
    return steps + [("merge", k) for k in range(K)]


def kernel(
    A, B, PODS,
    x_hbm, g_hbm, w_hbm, basis_hbm, err_hbm,
    out_ref, ne_ref,
    xv, xg, xt, gg, wq, bas, bz, ball, ev, eh, el, ysend, yrecv, up_s, up_r, dn_s, dn_r,
    ls, lz, left_s, left_r, zs, zr, rp, rq, rs, rw, rz, rown, rall, own,
    in_sem, send_sem, recv_sem, gs_sem, gr_sem, yr_sem, rs_sem, rr_sem,
):
    o = lax.axis_index("outer")
    c = lax.axis_index("chip")
    a, b = c // B, c % B
    T = x_hbm.shape[0]
    S, N = w_hbm.shape
    Q = B * S
    R = basis_hbm.shape[0]
    K = CHUNKS
    CN = N // K
    NP = N // PODS
    cols = [pl.ds(k * CN, CN) for k in range(K)]

    def rows_of(s):
        return pl.ds(pl.multiple_of(s * T, T), T)

    def shard_of(s):
        return pl.ds(pl.multiple_of(s * S, S), S)

    def share_of(s):
        return pl.ds(pl.multiple_of(s * NP, NP), NP)

    ins = [
        pltpu.make_async_copy(src, dst, in_sem.at[i])
        for i, (src, dst) in enumerate([
            (basis_hbm.at[:, share_of(o)], bz.at[a]),
            (x_hbm, xv),
            (g_hbm, gg.at[rows_of(a)]),
            (w_hbm, wq.at[shard_of(b)]),
            (basis_hbm, bas),
            (x_hbm.at[:, pl.ds(pl.multiple_of(a * Q, Q), Q)], xg.at[rows_of(a)]),
            (err_hbm, ev),
        ])
    ]
    for cp in ins:
        cp.start()

    line = [((a + d) % A) * B + b for d in range(1, A)]
    group = [(do, db) for do in range(PODS) for db in range(B) if do or db]

    def member(do, db):
        return {"outer": (o + do) % PODS, "chip": a * B + (b + db) % B}

    def remote(src, dst, ss, rs, where):
        return pltpu.make_async_remote_copy(
            src_ref=src, dst_ref=dst, send_sem=ss, recv_sem=rs,
            device_id=where, device_id_type=pl.DeviceIdType.MESH,
        )

    barrier = pltpu.get_barrier_semaphore()
    for t in line:
        pl.semaphore_signal(
            barrier, inc=1, device_id={"chip": t}, device_id_type=pl.DeviceIdType.MESH
        )
    for do, db in group:
        pl.semaphore_signal(
            barrier, inc=1, device_id=member(do, db), device_id_type=pl.DeviceIdType.MESH
        )
    pl.semaphore_wait(barrier, len(line) + len(group))

    def family(name, step=0):
        i = FAMILIES.index(name)
        return send_sem.at[i], recv_sem.at[i + step]

    def along(src, dst, name):
        return [
            remote(src((a + d) % A), dst, *family(name), {"chip": ((a + d) % A) * B + b})
            for d in range(1, A)
        ]

    def across(src, dst, name):
        return [
            remote(src(do, db), dst(j, db), *family(name), member(do, db))
            for j, (do, db) in enumerate(group)
        ]

    def whole(ref, name, step=0):
        return remote(ref, ref, *family(name, step), {"outer": (o + 1) % PODS})

    def start(copies):
        for cp in copies:
            cp.start()

    lines = pl.ds(0, A - 1)
    others = pl.ds(0, (PODS - 1) * NP)
    x_all = whole(xg.at[pl.ds(0, (A - 1) * T)], "x")
    c_all = whole(bz.at[lines], "c")
    v_all = whole(ball.at[pl.ds(0, B - 1), :, :, pl.ds(0, NP)], "v")
    b_all = whole(ball.at[:, :, :, others], "b")
    j_all = whole(ls.at[lines], "j")
    l_all = whole(left_r, "l")
    z_all = whole(zs.at[lines], "z")
    h_all = whole(rq, "h")
    t_all = whole(rs.at[lines], "t")
    p_all = whole(rown.at[:, others], "p")
    a_all = whole(rz.at[lines], "a")
    f_all = whole(rq, "f")
    y_all = whole(ysend, "y")

    x_copies = along(
        lambda t: xv.at[:, pl.ds(pl.multiple_of(t * Q, Q), Q)], xg.at[rows_of(a)], "x"
    )
    c_copies = along(lambda t: bz.at[a], bz.at[a], "c")
    b_copies = [
        [
            remote(
                bz if d == 0 else ball.at[d, :, :, share_of(o)],
                ball.at[d, :, :, share_of(o)],
                *family("b"), member(do, 0),
            )
            for do in range(1, PODS)
        ]
        for d in range(B)
    ]
    v_copies = [
        remote(bz, ball.at[(-d) % B, :, :, share_of(o)], *family("v"), member(0, d))
        for d in range(1, B)
    ]

    def g_copy(direction, h, k):
        step = 1 if direction == 0 else -1
        source = a - step * (h - 1)
        place = gg.at[rows_of(source), cols[k]]
        return remote(
            place, place, gs_sem.at[direction, h - 1], gr_sem.at[source, k],
            {"chip": c + step * B},
        )

    def g_sends(direction, h):
        return (
            jnp.logical_and(a - (h - 1) >= 0, a + 1 < A)
            if direction == 0
            else jnp.logical_and(a + (h - 1) < A, a >= 1)
        )

    def g_gets(direction, h):
        return a - h >= 0 if direction == 0 else a + h < A

    def g_arrival(direction, h, k):
        step = 1 if direction == 0 else -1
        source = a - step * h
        place = gg.at[rows_of(source), cols[k]]
        return remote(
            place, place, gs_sem.at[direction, h - 1], gr_sem.at[source, k],
            {"chip": c - step * B},
        )

    shared = PODS % 2 == 0
    mate = o + 1 - 2 * (o % 2)
    base, WN = (o % 2 * (N // 2), N // 2 // PIECES) if shared else (0, N // PIECES)
    w_copies, m_copies = [[] for _ in range(PIECES)], [[] for _ in range(PIECES)]
    for i in range(PIECES):
        piece = pl.ds(pl.multiple_of(base + i * WN, WN), WN)
        for d in range(1, B):
            here = wq.at[shard_of(b), piece]
            w_copies[i].append(remote(here, here, *family("w", i), member(0, d)))
            if shared:
                came = wq.at[shard_of((b - d + B) % B), piece]
                m_copies[i].append(remote(came, came, *family("m"), {"outer": mate}))
    rest = pl.ds(0, (B - 1) * S)
    w_part = [whole(wq.at[rest, pl.ds(0, WN)], "w", i) for i in range(PIECES)]
    w_all = whole(wq.at[rest, pl.ds(0, PIECES * WN)], "w")
    m_all = whole(wq.at[rest, pl.ds(0, PIECES * WN)], "m")

    def g_first(k):
        for direction in range(2):
            @pl.when(g_sends(direction, 1))
            def _():
                g_copy(direction, 1, k).start()

    ins[0].wait()
    start(c_copies)
    ins[1].wait()
    start(x_copies)
    ins[2].wait()
    for k in range(AHEAD):
        g_first(k)
    ins[3].wait()
    start(w_copies[0])
    for cp in ins[4:]:
        cp.wait()

    for k in range(K):
        high, low = halves(ev[:, cols[k]])
        eh[:, cols[k]] = high.astype(BF16)
        el[:, cols[k]] = low.astype(BF16)
    fed = thin_dot(bas[...], eh[...], el[...], 1)

    c_all.wait_recv()
    start(v_copies + b_copies[0])
    for copies in w_copies[1:]:
        start(copies)
    ball[0, :, :, share_of(o)] = bz[...]
    def y_copy(d, k):
        return remote(
            ysend.at[d - 1, :, cols[k]], yrecv.at[d - 1, :, cols[k]],
            family("y")[0], yr_sem.at[d - 1, k], member(0, d),
        )

    def gradient_chunk(k):
        for d in range(1, B):
            part = dot(xt[shard_of((b + d) % B), :], gg[:, cols[k]], 1, 0)
            ysend[d - 1, :, cols[k]] = part.astype(BF16)
            y_copy(d, k).start()
        ne_ref[:, cols[k]] = dot(xt[shard_of(b), :], gg[:, cols[k]], 1, 0)

    def merge_chunk(k):
        part = ne_ref[:, cols[k]]
        for d in range(1, B):
            y_copy(d, k).wait_recv()
            part = part + yrecv[d - 1, :, cols[k]].astype(F32)
        ne_ref[:, cols[k]] = part / TOK_DEV + ev[:, cols[k]]

    def o_copy(direction, r, k):
        s_buf, r_buf = (up_s, up_r) if direction == 0 else (dn_s, dn_r)
        return remote(
            s_buf.at[r - 1, :, cols[k]], r_buf.at[r - 1, :, cols[k]],
            rs_sem.at[direction, r - 1], rr_sem.at[a + r + 1 if direction == 0 else a - r, k],
            {"chip": c + B if direction == 0 else c - B},
        )

    def o_arrival(direction, r, k):
        r_buf = up_r if direction == 0 else dn_r
        place = r_buf.at[r - 1, :, cols[k]]
        return remote(
            place, place, rs_sem.at[direction, r - 1],
            rr_sem.at[a + r if direction == 0 else a + 1 - r, k],
            {"chip": c - B if direction == 0 else c + B},
        )

    def o_first(direction):
        return a == 0 if direction == 0 else a == A - 1

    def o_sends(direction, r):
        return a + r < A if direction == 0 else a - r >= 0

    def o_gets(direction, r):
        if direction == 0:
            return jnp.logical_and(a >= 1, a - 1 + r < A)
        return jnp.logical_and(a + 1 < A, a + 1 - r >= 0)

    def out_piece(direction, r, k, first):
        s_buf, r_buf = (up_s, up_r) if direction == 0 else (dn_s, dn_r)
        leads = o_first(direction)
        if not first:
            leads = jnp.logical_not(leads)

        @pl.when(jnp.logical_and(o_sends(direction, r), leads))
        def _():
            token = a + r if direction == 0 else a - r
            part = dot(xg[rows_of(token), :], wq[:, cols[k]], 1, 0)
            if not first:
                o_arrival(direction, r + 1, k).wait_recv()
                part = part + r_buf[r, :, cols[k]].astype(F32)
            s_buf[r - 1, :, cols[k]] = part.astype(BF16)
            o_copy(direction, r, k).start()

    def basis_pass():
        v_all.wait_recv()
        for d in range(1, B):
            start(b_copies[d])

    def left_part():
        b_all.wait_recv()
        thin = jnp.zeros((B * A * R, T), F32)
        for k in range(K):
            basis = split(jnp.concatenate(
                [ball[d, t, :, cols[k]] for d in range(B) for t in range(A)], axis=0
            ))
            thin = thin + fold(dot(basis, gg[rows_of(a), cols[k]], 1, 1))
        for d in range(B):
            for t in range(A):
                row = (d * A + t) * R
                shard = shard_of(t * B + (b + d) % B)
                ls[t, d] = fold(dot(split(thin[row : row + R, :]), xv[:, shard], 1, 0)) / TOK_DEV
        start(j_copies)
        lz[a] = ls[a]


    def x_in():
        x_all.wait_recv()
        xt[...] = xg[...].T

    def weights_in():
        for came, passed in zip(w_part, m_copies):
            came.wait_recv()
            start(passed)

    def mates_in():
        if shared:
            m_all.wait_recv()

    def first_piece(r, k):
        for direction in range(2):
            out_piece(direction, r, k, True)

    def rest_piece(r, k):
        for direction in range(2):
            out_piece(direction, r, k, False)

    j_copies = along(lambda t: ls.at[t], lz.at[a], "j")
    l_copies = across(lambda do, db: left_s, lambda j, db: left_r.at[j], "l")
    z_copies = along(lambda t: zs.at[t], zr.at[a], "z")
    h_copies = across(
        lambda do, db: rp.at[db, :, :, share_of((o + do) % PODS)],
        lambda j, db: rq.at[j], "h",
    )
    t_copies = along(lambda t: rs.at[t], rw.at[a], "t")
    a_copies = along(lambda t: rz.at[a], rz.at[a], "a")
    p_copies = [
        remote(rz.at[a], rown.at[:, share_of(o)], *family("p"), member(do, 0))
        for do in range(1, PODS)
    ]
    f_copies = across(
        lambda do, db: rz, lambda j, db: rall.at[(-db) % B, :, :, share_of(o)], "f"
    )

    def left_line():
        j_all.wait_recv()
        for d in range(B):
            part = lz[0, d]
            for t in range(1, A):
                part = part + lz[t, d]
            left_s[d] = part + fed if d == 0 else part
        start(l_copies)

    left = []

    def left_done():
        total = [left_s[d] for d in range(B)]
        l_all.wait_recv()
        for j, (do, db) in enumerate(group):
            for d in range(B):
                total[d] = total[d] + left_r[j, (d + db) % B]
        left.extend(orthonormal(total[d] / PODS) for d in range(B))
        z = jnp.concatenate(
            [fold(dot(split(left[d]), xt[shard_of((b + d) % B), :], 1, 0)) for d in range(B)],
            axis=0,
        )
        for t in range(A):
            zs[t] = z[:, t * T : (t + 1) * T]
        start(z_copies)
        zr[a] = zs[a]

    z_wide = []

    def right_part():
        z_all.wait_recv()
        z_wide.append(split(jnp.concatenate(
            [zr[t, d * R : (d + 1) * R, :] for d in range(B) for t in range(A)], axis=0
        )))
        for k in range(K):
            part = fold(dot(z_wide[0], gg[rows_of(a), cols[k]], 1, 0)) / TOK_DEV
            lead = thin_dot(left[0], eh[:, cols[k]], el[:, cols[k]], 0)
            for d in range(B):
                for t in range(A):
                    row = (d * A + t) * R
                    piece = part[row : row + R]
                    if d == 0:
                        piece = piece + jnp.where(a == t, lead, 0.0)
                    rp[d, t, :, cols[k]] = piece.astype(BF16)
        start(h_copies)

    def right_group():
        right = rp[0, :, :, share_of(o)].astype(F32)
        h_all.wait_recv()
        for j in range(len(group)):
            right = right + rq[j].astype(F32)
        rs[...] = right.astype(BF16)
        start(t_copies)
        rw[a] = rs[a]

    def right_line():
        t_all.wait_recv()
        right = rw[0].astype(F32)
        for t in range(1, A):
            right = right + rw[t].astype(F32)
        rz[a] = (right / PODS).astype(BF16)
        start(a_copies + p_copies)
        rown[:, share_of(o)] = rz[a]

    def right_all():
        a_all.wait_recv()
        start(f_copies)
        rall[0, :, :, share_of(o)] = rz[...]

    def own_out():
        for k in range(K):
            own[:, cols[k]] = dot(xg[rows_of(a), :], wq[:, cols[k]], 1, 0)

    def wave(step):
        for h in range(1, A):
            k = step - h
            if 0 <= k < K:
                for direction in range(2):
                    @pl.when(g_gets(direction, h))
                    def _():
                        g_arrival(direction, h, k).wait_recv()
                    if h + 1 < A:
                        @pl.when(g_sends(direction, h + 1))
                        def _():
                            g_copy(direction, h + 1, k).start()
        k = step - 1 + AHEAD
        if k < K:
            g_first(k)
        k = step - (A - 1)
        if 0 <= k < K:
            gradient_chunk(k)

    actions = {
        "basis": basis_pass, "left0": left_part, "x": x_in, "wave": wave, "weights": weights_in, "mates": mates_in, "left1": left_line,
        "left2": left_done, "right1": right_part, "right2": right_group,
        "right3": right_line, "right4": right_all, "own": own_out,
        "first": first_piece, "rest": rest_piece, "merge": merge_chunk,
    }
    for kind, *args in plan_of(A, K):
        actions[kind](*args)

    p_all.wait_recv()
    lefts = split(left[0])
    for k in range(K):
        mine = rown[:, cols[k]].astype(F32)
        ne_ref[:, cols[k]] = ne_ref[:, cols[k]] - dot(lefts, stack(mine, mine), 0, 0)

    f_all.wait_recv()
    for k in range(K):
        rights = jnp.concatenate(
            [rall[d, t, :, cols[k]].astype(F32) for d in range(B) for t in range(A)], axis=0
        )
        delta = dot(z_wide[0], stack(rights, rights), 0, 0)
        for direction in range(2):
            r_buf = up_r if direction == 0 else dn_r

            @pl.when(o_gets(direction, 1))
            def _():
                o_arrival(direction, 1, k).wait_recv()

            @pl.when(jnp.logical_not(o_gets(direction, 1)))
            def _():
                r_buf[0, :, cols[k]] = jnp.zeros((T, CN), BF16)
        mine = own[:, cols[k]] + up_r[0, :, cols[k]].astype(F32) + dn_r[0, :, cols[k]].astype(F32)
        out_ref[:, cols[k]] = (mine - LEARNING_RATE * delta).astype(BF16)

    for cp in (
        x_all, c_all, v_all, b_all, w_all, j_all, l_all, z_all, h_all, t_all, p_all, a_all, f_all,
        y_all,
    ):
        cp.wait_send()
    if shared:
        m_all.wait_send()
    for direction in range(2):
        for h in range(1, A):
            step = 1 if direction == 0 else -1

            @pl.when(g_sends(direction, h))
            def _():
                place = gg.at[rows_of(a - step * (h - 1))]
                remote(
                    place, place, gs_sem.at[direction, h - 1], gr_sem.at[0, 0],
                    {"chip": c + step * B},
                ).wait_send()

            @pl.when(o_sends(direction, h))
            def _():
                place = (up_s if direction == 0 else dn_s).at[h - 1]
                remote(
                    place, place, rs_sem.at[direction, h - 1], rr_sem.at[0, 0],
                    {"chip": c + step * B},
                ).wait_send()


def shards(inputs, out_grads, weight, start_basis, error_buffer):
    PODS, NC = lax.axis_size("outer"), lax.axis_size("chip")
    A = 4 if NC % 4 == 0 else NC
    B = NC // A
    T, D = inputs.shape
    N = out_grads.shape[1]
    S = weight.shape[0]
    R = start_basis.shape[0]
    Q = B * S
    K = CHUNKS
    G = PODS * B
    dma = pltpu.SemaphoreType.DMA
    vmem = pl.BlockSpec(memory_space=pltpu.VMEM)
    hbm = pl.BlockSpec(memory_space=pltpu.HBM)
    outputs, new_error = pl.pallas_call(
        functools.partial(kernel, A, B, PODS),
        out_shape=(
            pltpu.VMEM((T, N), BF16),
            pltpu.VMEM((S, N), F32),
        ),
        in_specs=[hbm] * 5,
        out_specs=(vmem, vmem),
        scratch_shapes=[
            pltpu.VMEM((T, D), BF16),
            pltpu.VMEM((A * T, Q), BF16),
            pltpu.VMEM((Q, A * T), BF16),
            pltpu.VMEM((A * T, N), BF16),
            pltpu.VMEM((Q, N), BF16),
            pltpu.VMEM((R, N), F32),
            pltpu.VMEM((A, R, N // PODS), F32),
            pltpu.VMEM((B, A, R, N), F32),
            pltpu.VMEM((S, N), F32),
            pltpu.VMEM((S, N), BF16),
            pltpu.VMEM((S, N), BF16),
            pltpu.VMEM((B - 1, S, N), BF16),
            pltpu.VMEM((B - 1, S, N), BF16),
            pltpu.VMEM((A - 1, T, N), BF16),
            pltpu.VMEM((A - 1, T, N), BF16),
            pltpu.VMEM((A - 1, T, N), BF16),
            pltpu.VMEM((A - 1, T, N), BF16),
            pltpu.VMEM((A, B, R, S), F32),
            pltpu.VMEM((A, B, R, S), F32),
            pltpu.VMEM((B, R, S), F32),
            pltpu.VMEM((G - 1, B, R, S), F32),
            pltpu.VMEM((A, B * R, T), F32),
            pltpu.VMEM((A, B * R, T), F32),
            pltpu.VMEM((B, A, R, N), BF16),
            pltpu.VMEM((G - 1, A, R, N // PODS), BF16),
            pltpu.VMEM((A, R, N // PODS), BF16),
            pltpu.VMEM((A, R, N // PODS), BF16),
            pltpu.VMEM((A, R, N // PODS), BF16),
            pltpu.VMEM((R, N), BF16),
            pltpu.VMEM((B, A, R, N), BF16),
            pltpu.VMEM((T, N), F32),
            dma((7,)), dma((len(FAMILIES),)), dma((len(FAMILIES) + PIECES - 1,)),
            dma((2, A - 1)), dma((A, K)), dma((B - 1, K)), dma((2, A - 1)), dma((A + 1, K)),
        ],
        compiler_params=pltpu.CompilerParams(
            collective_id=0, has_side_effects=True, vmem_limit_bytes=40 * 1024 * 1024
        ),
        name="step",
    )(*[
        pltpu.with_memory_space_constraint(t, pltpu.HBM)
        for t in (inputs, out_grads, weight, start_basis, error_buffer[0])
    ])
    return outputs, new_error[None]


def solution(mesh):
    return jax.shard_map(
        shards,
        mesh=mesh,
        in_specs=(
            P(("outer", "chip"), None),
            P(("outer", "chip"), None),
            P("chip", None),
            P("chip", None),
            P("outer", "chip", None),
        ),
        out_specs=(P(("outer", "chip"), None), P("outer", "chip", None)),
        check_vma=False,
    )
```

```python
import functools

import jax
import jax.numpy as jnp
from jax import lax
from jax.experimental import pallas as pl
from jax.experimental.pallas import tpu as pltpu
from jax.sharding import PartitionSpec as P

TOK_DEV = 128
LEARNING_RATE = 0.2
CHUNKS = 8
AHEAD = 4
PIECES = 2
FAMILIES = "abcfhjlmptvxyzw"
F32 = jnp.float32
BF16 = jnp.bfloat16


def dot(a, b, ca, cb):
    return lax.dot_general(
        a, b, (((ca,), (cb,)), ((), ())), preferred_element_type=F32
    )


def halves(v):
    high = v.astype(BF16).astype(F32)
    return high, v - high


def stack(*parts):
    return jnp.concatenate(parts, axis=0).astype(BF16)


def split(thin):
    return stack(*halves(thin))


def fold(both):
    n = both.shape[0] // 2
    return both[:n] + both[n:]


def thin_dot(thin, wide_high, wide_low, cb):
    n = thin.shape[0]
    both = split(thin)
    return fold(dot(both, wide_high, 1, cb)) + dot(both[:n], wide_low, 1, cb)


def orthonormal(v):
    count = v.shape[0]
    row = lax.broadcasted_iota(jnp.int32, (count, 1), 0)
    for k in range(count):
        pivot = v[k : k + 1, :]
        d = jnp.sum(v * pivot, axis=1, keepdims=True)
        norm = d[k : k + 1, :] + 1.0
        scale = jnp.where(row > k, d / norm, 0.0)
        unit = pivot / jnp.sqrt(norm)
        v = jnp.where(row == k, unit, v - scale * pivot)
    return v


PLAN = (
    ("basis",), ("send", 1), ("hop", 1, 1), ("left0",), ("x",), ("hop", 1, 1), ("send", 1),
    ("hop", 1, 1), ("send", 1), ("hop", 2, 1), ("weights",), ("hop", 1, 1), ("send",),
    ("hop", 2, 1), ("mates",), ("first", 3), ("grad",), ("hop", 1, 1), ("left1",), ("first", 3),
    ("hop", 2, 1), ("grad",), ("hop", 1, 1), ("left2",), ("own",), ("hop", 2, 1), ("hop", 1, 1),
    ("first", 4), ("grad",), ("hop", 1, 1), ("hop", 2, 1), ("rest", 2), ("right1",), ("first", 2),
    ("grad",), ("hop", 2, 1), ("rest", 3), ("first", 1), ("grad",), ("right2",), ("hop", 2, 1),
    ("rest", 3), ("first", 4), ("grad",), ("hop", 2, 1), ("outer", 2), ("first", 1), ("right3",),
    ("grad",), ("rest", 3), ("first", 3), ("outer", 3), ("grad",), ("rest", 2), ("right4",),
    ("first",), ("outer",), ("rest",), ("y",), ("merge",),
)


def plan_of(A, K):
    send = [("send", k) for k in range(AHEAD, K)]
    hops = [[("hop", h, k) for k in range(K)] for h in range(1, A)]
    grads = list(range(K))
    firsts = [("first", r, k) for r in range(A - 1, 0, -1) for k in range(K)]
    rests = [("rest", r, k) for r in range(A - 2, 1, -1) for k in range(K)]
    rests += [("inner", k) for k in range(K)]
    outers = [("outer", k) for k in range(K)]
    merges = [("merge", k) for k in range(K)]
    queues = {"send": send, "first": firsts, "rest": rests, "outer": outers, "merge": merges}
    steps = []

    def take(queue, count):
        steps.extend(queue[:count])
        del queue[:count]

    def gradient():
        k = grads.pop(0)
        for h in range(1, A):
            take(hops[h - 1], K - len(hops[h - 1]) <= k and k + 1 - (K - len(hops[h - 1])))
        steps.append(("grad", k))

    for kind, *args in PLAN:
        if kind == "hop":
            h, count = args
            if h < A:
                take(hops[h - 1], count)
        elif kind == "grad":
            if grads:
                gradient()
        elif kind in queues:
            take(queues[kind], args[0] if args else len(queues[kind]))
        else:
            if kind == "right4":
                take(send, K)
                while grads:
                    gradient()
            steps.append((kind,))
    return steps


def kernel(
    A, B, PODS,
    x_hbm, g_hbm, w_hbm, basis_hbm, err_hbm,
    out_ref, ne_ref,
    xv, xg, xt, gg, wq, bas, bz, ball, ev, eh, el, ysend, yrecv, up_s, up_r, dn_s, dn_r,
    ls, lz, left_s, left_r, zs, zr, rp, rq, rs, rw, rz, rown, rall, own,
    in_sem, send_sem, recv_sem, gs_sem, gr_sem, rs_sem, rr_sem,
):
    o = lax.axis_index("outer")
    c = lax.axis_index("chip")
    a, b = c // B, c % B
    T = x_hbm.shape[0]
    S, N = w_hbm.shape
    Q = B * S
    R = basis_hbm.shape[0]
    K = CHUNKS
    CN = N // K
    NP = N // PODS
    cols = [pl.ds(k * CN, CN) for k in range(K)]

    def rows_of(s):
        return pl.ds(pl.multiple_of(s * T, T), T)

    def shard_of(s):
        return pl.ds(pl.multiple_of(s * S, S), S)

    def share_of(s):
        return pl.ds(pl.multiple_of(s * NP, NP), NP)

    ins = [
        pltpu.make_async_copy(src, dst, in_sem.at[i])
        for i, (src, dst) in enumerate([
            (basis_hbm.at[:, share_of(o)], bz.at[a]),
            (x_hbm, xv),
            (g_hbm, gg.at[rows_of(a)]),
            (w_hbm, wq.at[shard_of(b)]),
            (basis_hbm, bas),
            (x_hbm.at[:, pl.ds(pl.multiple_of(a * Q, Q), Q)], xg.at[rows_of(a)]),
            (err_hbm, ev),
        ])
    ]
    for cp in ins:
        cp.start()

    line = [((a + d) % A) * B + b for d in range(1, A)]
    group = [(do, db) for do in range(PODS) for db in range(B) if do or db]

    def member(do, db):
        return {"outer": (o + do) % PODS, "chip": a * B + (b + db) % B}

    def remote(src, dst, ss, rs, where):
        return pltpu.make_async_remote_copy(
            src_ref=src, dst_ref=dst, send_sem=ss, recv_sem=rs,
            device_id=where, device_id_type=pl.DeviceIdType.MESH,
        )

    barrier = pltpu.get_barrier_semaphore()
    for t in line:
        pl.semaphore_signal(
            barrier, inc=1, device_id={"chip": t}, device_id_type=pl.DeviceIdType.MESH
        )
    for do, db in group:
        pl.semaphore_signal(
            barrier, inc=1, device_id=member(do, db), device_id_type=pl.DeviceIdType.MESH
        )
    pl.semaphore_wait(barrier, len(line) + len(group))

    def family(name, step=0):
        i = FAMILIES.index(name)
        return send_sem.at[i], recv_sem.at[i + step]

    def along(src, dst, name):
        return [
            remote(src((a + d) % A), dst, *family(name), {"chip": ((a + d) % A) * B + b})
            for d in range(1, A)
        ]

    def across(src, dst, name):
        return [
            remote(src(do, db), dst(j, db), *family(name), member(do, db))
            for j, (do, db) in enumerate(group)
        ]

    def whole(ref, name, step=0):
        return remote(ref, ref, *family(name, step), {"outer": (o + 1) % PODS})

    def start(copies):
        for cp in copies:
            cp.start()

    lines = pl.ds(0, A - 1)
    others = pl.ds(0, (PODS - 1) * NP)
    x_all = whole(xg.at[pl.ds(0, (A - 1) * T)], "x")
    c_all = whole(bz.at[lines], "c")
    v_all = whole(ball.at[pl.ds(0, B - 1), :, :, pl.ds(0, NP)], "v")
    b_all = whole(ball.at[:, :, :, others], "b")
    j_all = whole(ls.at[lines], "j")
    l_all = whole(left_r, "l")
    z_all = whole(zs.at[lines], "z")
    h_all = whole(rq, "h")
    t_all = whole(rs.at[lines], "t")
    p_all = whole(rown.at[:, others], "p")
    a_all = whole(rz.at[lines], "a")
    f_all = whole(rq, "f")
    y_all = whole(ysend, "y")

    x_copies = along(
        lambda t: xv.at[:, pl.ds(pl.multiple_of(t * Q, Q), Q)], xg.at[rows_of(a)], "x"
    )
    c_copies = along(lambda t: bz.at[a], bz.at[a], "c")
    b_copies = [
        [
            remote(
                bz if d == 0 else ball.at[d, :, :, share_of(o)],
                ball.at[d, :, :, share_of(o)],
                *family("b"), member(do, 0),
            )
            for do in range(1, PODS)
        ]
        for d in range(B)
    ]
    v_copies = [
        remote(bz, ball.at[(-d) % B, :, :, share_of(o)], *family("v"), member(0, d))
        for d in range(1, B)
    ]

    def g_copy(direction, h, k):
        step = 1 if direction == 0 else -1
        source = a - step * (h - 1)
        place = gg.at[rows_of(source), cols[k]]
        return remote(
            place, place, gs_sem.at[direction, h - 1], gr_sem.at[source, k],
            {"chip": c + step * B},
        )

    def g_sends(direction, h):
        return (
            jnp.logical_and(a - (h - 1) >= 0, a + 1 < A)
            if direction == 0
            else jnp.logical_and(a + (h - 1) < A, a >= 1)
        )

    def g_gets(direction, h):
        return a - h >= 0 if direction == 0 else a + h < A

    def g_arrival(direction, h, k):
        step = 1 if direction == 0 else -1
        source = a - step * h
        place = gg.at[rows_of(source), cols[k]]
        return remote(
            place, place, gs_sem.at[direction, h - 1], gr_sem.at[source, k],
            {"chip": c - step * B},
        )

    shared = PODS % 2 == 0
    mate = o + 1 - 2 * (o % 2)
    base, WN = (o % 2 * (N // 2), N // 2 // PIECES) if shared else (0, N // PIECES)
    w_copies, m_copies = [[] for _ in range(PIECES)], [[] for _ in range(PIECES)]
    for i in range(PIECES):
        piece = pl.ds(pl.multiple_of(base + i * WN, WN), WN)
        for d in range(1, B):
            here = wq.at[shard_of(b), piece]
            w_copies[i].append(remote(here, here, *family("w", i), member(0, d)))
            if shared:
                came = wq.at[shard_of((b - d + B) % B), piece]
                m_copies[i].append(remote(came, came, *family("m"), {"outer": mate}))
    rest = pl.ds(0, (B - 1) * S)
    w_part = [whole(wq.at[rest, pl.ds(0, WN)], "w", i) for i in range(PIECES)]
    w_all = whole(wq.at[rest, pl.ds(0, PIECES * WN)], "w")
    m_all = whole(wq.at[rest, pl.ds(0, PIECES * WN)], "m")

    def g_first(k):
        for direction in range(2):
            @pl.when(g_sends(direction, 1))
            def _():
                g_copy(direction, 1, k).start()

    ins[0].wait()
    start(c_copies)
    ins[1].wait()
    start(x_copies)
    ins[2].wait()
    for k in range(AHEAD):
        g_first(k)
    ins[3].wait()
    start(w_copies[0])
    for cp in ins[4:]:
        cp.wait()

    for k in range(K):
        high, low = halves(ev[:, cols[k]])
        eh[:, cols[k]] = high.astype(BF16)
        el[:, cols[k]] = low.astype(BF16)
    fed = thin_dot(bas[...], eh[...], el[...], 1)

    c_all.wait_recv()
    start(v_copies + b_copies[0])
    for copies in w_copies[1:]:
        start(copies)
    ball[0, :, :, share_of(o)] = bz[...]
    def y_copy(d, k):
        return remote(
            ysend.at[d - 1, :, cols[k]], yrecv.at[d - 1, :, cols[k]],
            *family("y"), member(0, d),
        )

    def gradient_chunk(k):
        for d in range(1, B):
            part = dot(xt[shard_of((b + d) % B), :], gg[:, cols[k]], 1, 0)
            ysend[d - 1, :, cols[k]] = part.astype(BF16)
            y_copy(d, k).start()
        ne_ref[:, cols[k]] = dot(xt[shard_of(b), :], gg[:, cols[k]], 1, 0)

    def y_in():
        y_all.wait_recv()

    def merge_chunk(k):
        part = ne_ref[:, cols[k]]
        for d in range(1, B):
            part = part + yrecv[d - 1, :, cols[k]].astype(F32)
        ne_ref[:, cols[k]] = part / TOK_DEV + ev[:, cols[k]]

    def o_copy(direction, r, k):
        s_buf, r_buf = (up_s, up_r) if direction == 0 else (dn_s, dn_r)
        return remote(
            s_buf.at[r - 1, :, cols[k]], r_buf.at[r - 1, :, cols[k]],
            rs_sem.at[direction, r - 1], rr_sem.at[a + r + 1 if direction == 0 else a - r, k],
            {"chip": c + B if direction == 0 else c - B},
        )

    def o_arrival(direction, r, k):
        r_buf = up_r if direction == 0 else dn_r
        place = r_buf.at[r - 1, :, cols[k]]
        return remote(
            place, place, rs_sem.at[direction, r - 1],
            rr_sem.at[a + r if direction == 0 else a + 1 - r, k],
            {"chip": c - B if direction == 0 else c + B},
        )

    def o_first(direction):
        return a == 0 if direction == 0 else a == A - 1

    def o_sends(direction, r):
        return a + r < A if direction == 0 else a - r >= 0

    def o_gets(direction, r):
        if direction == 0:
            return jnp.logical_and(a >= 1, a - 1 + r < A)
        return jnp.logical_and(a + 1 < A, a + 1 - r >= 0)

    def o_outer(direction):
        return a == A - 2 if direction == 0 else a == 1

    def out_piece(direction, r, k, first, outer=None):
        s_buf, r_buf = (up_s, up_r) if direction == 0 else (dn_s, dn_r)
        leads = o_first(direction)
        if not first:
            leads = jnp.logical_not(leads)
        if outer is not None:
            bound = o_outer(direction)
            leads = jnp.logical_and(leads, bound if outer else jnp.logical_not(bound))

        @pl.when(jnp.logical_and(o_sends(direction, r), leads))
        def _():
            token = a + r if direction == 0 else a - r
            part = dot(xg[rows_of(token), :], wq[:, cols[k]], 1, 0)
            if not first:
                o_arrival(direction, r + 1, k).wait_recv()
                part = part + r_buf[r, :, cols[k]].astype(F32)
            s_buf[r - 1, :, cols[k]] = part.astype(BF16)
            o_copy(direction, r, k).start()

    def basis_pass():
        v_all.wait_recv()
        for d in range(1, B):
            start(b_copies[d])

    def left_part():
        b_all.wait_recv()
        thin = jnp.zeros((B * A * R, T), F32)
        for k in range(K):
            basis = split(jnp.concatenate(
                [ball[d, t, :, cols[k]] for d in range(B) for t in range(A)], axis=0
            ))
            thin = thin + fold(dot(basis, gg[rows_of(a), cols[k]], 1, 1))
        for d in range(B):
            for t in range(A):
                row = (d * A + t) * R
                shard = shard_of(t * B + (b + d) % B)
                ls[t, d] = fold(dot(split(thin[row : row + R, :]), xv[:, shard], 1, 0)) / TOK_DEV
        start(j_copies)
        lz[a] = ls[a]


    def x_in():
        x_all.wait_recv()
        xt[...] = xg[...].T

    def weights_in():
        for came, passed in zip(w_part, m_copies):
            came.wait_recv()
            start(passed)

    def mates_in():
        if shared:
            m_all.wait_recv()

    def first_piece(r, k):
        for direction in range(2):
            out_piece(direction, r, k, True)

    def rest_piece(r, k):
        for direction in range(2):
            out_piece(direction, r, k, False)

    j_copies = along(lambda t: ls.at[t], lz.at[a], "j")
    def inner_piece(k):
        for direction in range(2):
            out_piece(direction, 1, k, False, False)

    def outer_piece(k):
        for direction in range(2):
            out_piece(direction, 1, k, False, True)

    l_copies = across(lambda do, db: left_s, lambda j, db: left_r.at[j], "l")
    z_copies = along(lambda t: zs.at[t], zr.at[a], "z")
    h_copies = across(
        lambda do, db: rp.at[db, :, :, share_of((o + do) % PODS)],
        lambda j, db: rq.at[j], "h",
    )
    t_copies = along(lambda t: rs.at[t], rw.at[a], "t")
    a_copies = along(lambda t: rz.at[a], rz.at[a], "a")
    p_copies = [
        remote(rz.at[a], rown.at[:, share_of(o)], *family("p"), member(do, 0))
        for do in range(1, PODS)
    ]
    f_copies = across(
        lambda do, db: rz, lambda j, db: rall.at[(-db) % B, :, :, share_of(o)], "f"
    )

    def left_line():
        j_all.wait_recv()
        for d in range(B):
            part = lz[0, d]
            for t in range(1, A):
                part = part + lz[t, d]
            left_s[d] = part + fed if d == 0 else part
        start(l_copies)

    left = []

    def left_done():
        total = [left_s[d] for d in range(B)]
        l_all.wait_recv()
        for j, (do, db) in enumerate(group):
            for d in range(B):
                total[d] = total[d] + left_r[j, (d + db) % B]
        left.extend(orthonormal(total[d] / PODS) for d in range(B))
        z = jnp.concatenate(
            [fold(dot(split(left[d]), xt[shard_of((b + d) % B), :], 1, 0)) for d in range(B)],
            axis=0,
        )
        for t in range(A):
            zs[t] = z[:, t * T : (t + 1) * T]
        start(z_copies)
        zr[a] = zs[a]

    z_wide = []

    def right_part():
        z_all.wait_recv()
        z_wide.append(split(jnp.concatenate(
            [zr[t, d * R : (d + 1) * R, :] for d in range(B) for t in range(A)], axis=0
        )))
        for k in range(K):
            part = fold(dot(z_wide[0], gg[rows_of(a), cols[k]], 1, 0)) / TOK_DEV
            lead = thin_dot(left[0], eh[:, cols[k]], el[:, cols[k]], 0)
            for d in range(B):
                for t in range(A):
                    row = (d * A + t) * R
                    piece = part[row : row + R]
                    if d == 0:
                        piece = piece + jnp.where(a == t, lead, 0.0)
                    rp[d, t, :, cols[k]] = piece.astype(BF16)
        start(h_copies)

    def right_group():
        right = rp[0, :, :, share_of(o)].astype(F32)
        h_all.wait_recv()
        for j in range(len(group)):
            right = right + rq[j].astype(F32)
        rs[...] = right.astype(BF16)
        start(t_copies)
        rw[a] = rs[a]

    def right_line():
        t_all.wait_recv()
        right = rw[0].astype(F32)
        for t in range(1, A):
            right = right + rw[t].astype(F32)
        rz[a] = (right / PODS).astype(BF16)
        start(a_copies + p_copies)
        rown[:, share_of(o)] = rz[a]

    def right_all():
        a_all.wait_recv()
        start(f_copies)
        rall[0, :, :, share_of(o)] = rz[...]

    def own_out():
        for k in range(K):
            own[:, cols[k]] = dot(xg[rows_of(a), :], wq[:, cols[k]], 1, 0)

    def hop(h, k):
        for direction in range(2):
            @pl.when(g_gets(direction, h))
            def _():
                g_arrival(direction, h, k).wait_recv()
            if h + 1 < A:
                @pl.when(g_sends(direction, h + 1))
                def _():
                    g_copy(direction, h + 1, k).start()

    def grad(k):
        gradient_chunk(k)

    actions = {
        "basis": basis_pass, "left0": left_part, "x": x_in, "send": g_first, "hop": hop,
        "grad": grad, "weights": weights_in, "mates": mates_in, "left1": left_line,
        "left2": left_done, "right1": right_part, "right2": right_group,
        "right3": right_line, "right4": right_all, "own": own_out,
        "first": first_piece, "rest": rest_piece,
        "inner": inner_piece, "outer": outer_piece, "y": y_in, "merge": merge_chunk,
    }
    for kind, *args in plan_of(A, K):
        actions[kind](*args)

    p_all.wait_recv()
    lefts = split(left[0])
    for k in range(K):
        mine = rown[:, cols[k]].astype(F32)
        ne_ref[:, cols[k]] = ne_ref[:, cols[k]] - dot(lefts, stack(mine, mine), 0, 0)

    f_all.wait_recv()
    for k in range(K):
        rights = jnp.concatenate(
            [rall[d, t, :, cols[k]].astype(F32) for d in range(B) for t in range(A)], axis=0
        )
        delta = dot(z_wide[0], stack(rights, rights), 0, 0)
        for direction in range(2):
            r_buf = up_r if direction == 0 else dn_r

            @pl.when(o_gets(direction, 1))
            def _():
                o_arrival(direction, 1, k).wait_recv()

            @pl.when(jnp.logical_not(o_gets(direction, 1)))
            def _():
                r_buf[0, :, cols[k]] = jnp.zeros((T, CN), BF16)
        mine = own[:, cols[k]] + up_r[0, :, cols[k]].astype(F32) + dn_r[0, :, cols[k]].astype(F32)
        out_ref[:, cols[k]] = (mine - LEARNING_RATE * delta).astype(BF16)

    for cp in (
        x_all, c_all, v_all, b_all, w_all, j_all, l_all, z_all, h_all, t_all, p_all, a_all, f_all,
        y_all,
    ):
        cp.wait_send()
    if shared:
        m_all.wait_send()
    for direction in range(2):
        for h in range(1, A):
            step = 1 if direction == 0 else -1

            @pl.when(g_sends(direction, h))
            def _():
                place = gg.at[rows_of(a - step * (h - 1))]
                remote(
                    place, place, gs_sem.at[direction, h - 1], gr_sem.at[0, 0],
                    {"chip": c + step * B},
                ).wait_send()

            @pl.when(o_sends(direction, h))
            def _():
                place = (up_s if direction == 0 else dn_s).at[h - 1]
                remote(
                    place, place, rs_sem.at[direction, h - 1], rr_sem.at[0, 0],
                    {"chip": c + step * B},
                ).wait_send()


def store(out_vmem, ne_vmem, out_hbm, ne_hbm, sem):
    copies = [
        pltpu.make_async_copy(ne_vmem, ne_hbm, sem.at[0]),
        pltpu.make_async_copy(out_vmem, out_hbm, sem.at[1]),
    ]
    for cp in copies:
        cp.start()
    for cp in copies:
        cp.wait()


def shards(inputs, out_grads, weight, start_basis, error_buffer):
    PODS, NC = lax.axis_size("outer"), lax.axis_size("chip")
    A = 4 if NC % 4 == 0 else NC
    B = NC // A
    T, D = inputs.shape
    N = out_grads.shape[1]
    S = weight.shape[0]
    R = start_basis.shape[0]
    Q = B * S
    K = CHUNKS
    G = PODS * B
    dma = pltpu.SemaphoreType.DMA
    vmem = pl.BlockSpec(memory_space=pltpu.VMEM)
    hbm = pl.BlockSpec(memory_space=pltpu.HBM)
    outputs, new_error = pl.pallas_call(
        functools.partial(kernel, A, B, PODS),
        out_shape=(
            pltpu.VMEM((T, N), BF16),
            pltpu.VMEM((S, N), F32),
        ),
        in_specs=[hbm] * 5,
        out_specs=(vmem, vmem),
        scratch_shapes=[
            pltpu.VMEM((T, D), BF16),
            pltpu.VMEM((A * T, Q), BF16),
            pltpu.VMEM((Q, A * T), BF16),
            pltpu.VMEM((A * T, N), BF16),
            pltpu.VMEM((Q, N), BF16),
            pltpu.VMEM((R, N), F32),
            pltpu.VMEM((A, R, N // PODS), F32),
            pltpu.VMEM((B, A, R, N), F32),
            pltpu.VMEM((S, N), F32),
            pltpu.VMEM((S, N), BF16),
            pltpu.VMEM((S, N), BF16),
            pltpu.VMEM((B - 1, S, N), BF16),
            pltpu.VMEM((B - 1, S, N), BF16),
            pltpu.VMEM((A - 1, T, N), BF16),
            pltpu.VMEM((A - 1, T, N), BF16),
            pltpu.VMEM((A - 1, T, N), BF16),
            pltpu.VMEM((A - 1, T, N), BF16),
            pltpu.VMEM((A, B, R, S), F32),
            pltpu.VMEM((A, B, R, S), F32),
            pltpu.VMEM((B, R, S), F32),
            pltpu.VMEM((G - 1, B, R, S), F32),
            pltpu.VMEM((A, B * R, T), F32),
            pltpu.VMEM((A, B * R, T), F32),
            pltpu.VMEM((B, A, R, N), BF16),
            pltpu.VMEM((G - 1, A, R, N // PODS), BF16),
            pltpu.VMEM((A, R, N // PODS), BF16),
            pltpu.VMEM((A, R, N // PODS), BF16),
            pltpu.VMEM((A, R, N // PODS), BF16),
            pltpu.VMEM((R, N), BF16),
            pltpu.VMEM((B, A, R, N), BF16),
            pltpu.VMEM((T, N), F32),
            dma((7,)), dma((len(FAMILIES),)), dma((len(FAMILIES) + PIECES - 1,)),
            dma((2, A - 1)), dma((A, K)), dma((2, A - 1)), dma((A + 1, K)),
        ],
        compiler_params=pltpu.CompilerParams(
            collective_id=0, has_side_effects=True, vmem_limit_bytes=40 * 1024 * 1024
        ),
        name="step",
    )(*[
        pltpu.with_memory_space_constraint(t, pltpu.HBM)
        for t in (inputs, out_grads, weight, start_basis, error_buffer[0])
    ])
    hbm_out = pl.BlockSpec(memory_space=pltpu.HBM)
    outputs, new_error = pl.pallas_call(
        store,
        out_shape=(
            jax.ShapeDtypeStruct((T, N), BF16),
            jax.ShapeDtypeStruct((S, N), F32),
        ),
        in_specs=[vmem] * 2,
        out_specs=(hbm_out, hbm_out),
        scratch_shapes=[dma((2,))],
        compiler_params=pltpu.CompilerParams(vmem_limit_bytes=8 * 1024 * 1024),
        name="store",
    )(outputs, new_error)
    return outputs, new_error[None]


def solution(mesh):
    return jax.shard_map(
        shards,
        mesh=mesh,
        in_specs=(
            P(("outer", "chip"), None),
            P(("outer", "chip"), None),
            P("chip", None),
            P("chip", None),
            P("outer", "chip", None),
        ),
        out_specs=(P(("outer", "chip"), None), P("outer", "chip", None)),
        check_vma=False,
    )
```

```python
import functools

import jax
import jax.numpy as jnp
from jax import lax
from jax.experimental import pallas as pl
from jax.experimental.pallas import tpu as pltpu
from jax.sharding import PartitionSpec as P

TOK_DEV = 128
LEARNING_RATE = 0.2
CHUNKS = 8
AHEAD = 4
PIECES = 2
FAMILIES = "abcfhjlmptvxyzw"
F32 = jnp.float32
BF16 = jnp.bfloat16


def dot(a, b, ca, cb):
    return lax.dot_general(
        a, b, (((ca,), (cb,)), ((), ())), preferred_element_type=F32
    )


def halves(v):
    high = v.astype(BF16).astype(F32)
    return high, v - high


def stack(*parts):
    return jnp.concatenate(parts, axis=0).astype(BF16)


def split(thin):
    return stack(*halves(thin))


def fold(both):
    n = both.shape[0] // 2
    return both[:n] + both[n:]


def thin_dot(thin, wide_high, wide_low, cb):
    n = thin.shape[0]
    both = split(thin)
    return fold(dot(both, wide_high, 1, cb)) + dot(both[:n], wide_low, 1, cb)


def orthonormal(v):
    count = v.shape[0]
    row = lax.broadcasted_iota(jnp.int32, (count, 1), 0)
    for k in range(count):
        pivot = v[k : k + 1, :]
        d = jnp.sum(v * pivot, axis=1, keepdims=True)
        norm = d[k : k + 1, :] + 1.0
        scale = jnp.where(row > k, d / norm, 0.0)
        unit = pivot / jnp.sqrt(norm)
        v = jnp.where(row == k, unit, v - scale * pivot)
    return v


PLAN = (
    ("hop", 1, 1), ("out", 1), ("basis",), ("out", 2), ("into", 1), ("x",), ("hop", 2, 1),
    ("hop", 1, 1), ("left0",), ("weights",), ("mates",), ("hop", 1, 1), ("into", 1),
    ("hop", 1, 1), ("first", 2), ("hop", 2, 1), ("hop", 1, 1), ("into", 1), ("first", 1),
    ("left1",), ("first", 1), ("rest", 1), ("first", 2), ("hop", 2, 1), ("grad",), ("left2",),
    ("rest", 1), ("hop", 1, 1), ("grad",), ("hop", 2, 1), ("into", 1), ("first", 2),
    ("hop", 2, 1), ("hop", 1, 1), ("rest", 2), ("first", 1), ("outer", 1), ("grad",),
    ("first", 1), ("right1",), ("rest", 1), ("first", 2), ("rest", 1), ("outer", 1), ("out", 1),
    ("grad",), ("hop", 2, 1), ("grad",), ("hop", 2, 1), ("right2",), ("first", 1), ("hop", 1, 1),
    ("first", 2), ("rest", 1), ("first", 1), ("rest", 1), ("own",), ("grad",), ("grad",),
    ("right3",), ("first", 2), ("hop", 2, 1), ("outer", 1), ("rest", 1), ("outer", 1),
    ("rest", 2), ("outer", 1), ("first", 3), ("outer", 1), ("first", 1), ("outer", 1),
    ("rest", 1), ("grad",), ("outer", 1), ("rest", 2), ("first", 1), ("rest", 2), ("first", 1),
    ("right4",), ("y",), ("merge",),
)


def plan_of(A, K):
    out = [("out", k) for k in range(AHEAD, K)]
    into = [("into", k) for k in range(AHEAD, K)]
    hops = [[("hop", h, k) for k in range(K)] for h in range(1, A)]
    grads = list(range(K))
    firsts = [("first", r, k) for r in range(A - 1, 0, -1) for k in range(K)]
    rests = [("rest", r, k) for r in range(A - 2, 1, -1) for k in range(K)]
    rests += [("inner", k) for k in range(K)]
    outers = [("outer", k) for k in range(K)]
    merges = [("merge", k) for k in range(K)]
    queues = {"out": out, "into": into, "first": firsts, "rest": rests, "outer": outers, "merge": merges}
    steps = []

    def take(queue, count):
        steps.extend(queue[:count])
        del queue[:count]

    def gradient():
        k = grads.pop(0)
        for h in range(1, A):
            take(hops[h - 1], K - len(hops[h - 1]) <= k and k + 1 - (K - len(hops[h - 1])))
        steps.append(("grad", k))

    for kind, *args in PLAN:
        if kind == "hop":
            h, count = args
            if h < A:
                take(hops[h - 1], count)
        elif kind == "grad":
            if grads:
                gradient()
        elif kind in queues:
            take(queues[kind], args[0] if args else len(queues[kind]))
        else:
            if kind == "y":
                take(out, K)
                take(into, K)
                while grads:
                    gradient()
            steps.append((kind,))
    return steps


def kernel(
    A, B, PODS,
    x_hbm, g_hbm, w_hbm, basis_hbm, err_hbm,
    out_ref, ne_ref,
    xv, xg, xt, gg, wq, bas, bz, ball, ev, eh, el, ysend, yrecv, up_s, up_r, dn_s, dn_r,
    ls, lz, left_s, left_r, zs, zr, rp, rq, rs, rw, rz, rown, rall, own,
    in_sem, send_sem, recv_sem, gs_sem, gr_sem, rs_sem, rr_sem,
):
    o = lax.axis_index("outer")
    c = lax.axis_index("chip")
    a, b = c // B, c % B
    T = x_hbm.shape[0]
    S, N = w_hbm.shape
    Q = B * S
    R = basis_hbm.shape[0]
    K = CHUNKS
    CN = N // K
    NP = N // PODS
    cols = [pl.ds(k * CN, CN) for k in range(K)]

    def rows_of(s):
        return pl.ds(pl.multiple_of(s * T, T), T)

    def shard_of(s):
        return pl.ds(pl.multiple_of(s * S, S), S)

    def share_of(s):
        return pl.ds(pl.multiple_of(s * NP, NP), NP)

    ins = [
        pltpu.make_async_copy(src, dst, in_sem.at[i])
        for i, (src, dst) in enumerate([
            (basis_hbm.at[:, share_of(o)], bz.at[a]),
            (x_hbm, xv),
            (g_hbm, gg.at[rows_of(a)]),
            (w_hbm, wq.at[shard_of(b)]),
            (basis_hbm, bas),
            (x_hbm.at[:, pl.ds(pl.multiple_of(a * Q, Q), Q)], xg.at[rows_of(a)]),
            (err_hbm, ev),
        ])
    ]
    for cp in ins:
        cp.start()

    line = [((a + d) % A) * B + b for d in range(1, A)]
    group = [(do, db) for do in range(PODS) for db in range(B) if do or db]

    def member(do, db):
        return {"outer": (o + do) % PODS, "chip": a * B + (b + db) % B}

    def remote(src, dst, ss, rs, where):
        return pltpu.make_async_remote_copy(
            src_ref=src, dst_ref=dst, send_sem=ss, recv_sem=rs,
            device_id=where, device_id_type=pl.DeviceIdType.MESH,
        )

    barrier = pltpu.get_barrier_semaphore()
    for t in line:
        pl.semaphore_signal(
            barrier, inc=1, device_id={"chip": t}, device_id_type=pl.DeviceIdType.MESH
        )
    for do, db in group:
        pl.semaphore_signal(
            barrier, inc=1, device_id=member(do, db), device_id_type=pl.DeviceIdType.MESH
        )
    pl.semaphore_wait(barrier, len(line) + len(group))

    def family(name, step=0):
        i = FAMILIES.index(name)
        return send_sem.at[i], recv_sem.at[i + step]

    def along(src, dst, name):
        return [
            remote(src((a + d) % A), dst, *family(name), {"chip": ((a + d) % A) * B + b})
            for d in range(1, A)
        ]

    def across(src, dst, name):
        return [
            remote(src(do, db), dst(j, db), *family(name), member(do, db))
            for j, (do, db) in enumerate(group)
        ]

    def whole(ref, name, step=0):
        return remote(ref, ref, *family(name, step), {"outer": (o + 1) % PODS})

    def start(copies):
        for cp in copies:
            cp.start()

    lines = pl.ds(0, A - 1)
    others = pl.ds(0, (PODS - 1) * NP)
    x_all = whole(xg.at[pl.ds(0, (A - 1) * T)], "x")
    c_all = whole(bz.at[lines], "c")
    v_all = whole(ball.at[pl.ds(0, B - 1), :, :, pl.ds(0, NP)], "v")
    b_all = whole(ball.at[:, :, :, others], "b")
    j_all = whole(ls.at[lines], "j")
    l_all = whole(left_r, "l")
    z_all = whole(zs.at[lines], "z")
    h_all = whole(rq, "h")
    t_all = whole(rs.at[lines], "t")
    p_all = whole(rown.at[:, others], "p")
    a_all = whole(rz.at[lines], "a")
    f_all = whole(rq, "f")
    y_all = whole(ysend, "y")

    x_copies = along(
        lambda t: xv.at[:, pl.ds(pl.multiple_of(t * Q, Q), Q)], xg.at[rows_of(a)], "x"
    )
    c_copies = along(lambda t: bz.at[a], bz.at[a], "c")
    b_copies = [
        [
            remote(
                bz if d == 0 else ball.at[d, :, :, share_of(o)],
                ball.at[d, :, :, share_of(o)],
                *family("b"), member(do, 0),
            )
            for do in range(1, PODS)
        ]
        for d in range(B)
    ]
    v_copies = [
        remote(bz, ball.at[(-d) % B, :, :, share_of(o)], *family("v"), member(0, d))
        for d in range(1, B)
    ]

    def g_copy(direction, h, k):
        step = 1 if direction == 0 else -1
        source = a - step * (h - 1)
        place = gg.at[rows_of(source), cols[k]]
        return remote(
            place, place, gs_sem.at[direction, h - 1], gr_sem.at[source, k],
            {"chip": c + step * B},
        )

    def g_sends(direction, h):
        return (
            jnp.logical_and(a - (h - 1) >= 0, a + 1 < A)
            if direction == 0
            else jnp.logical_and(a + (h - 1) < A, a >= 1)
        )

    def g_gets(direction, h):
        return a - h >= 0 if direction == 0 else a + h < A

    def g_arrival(direction, h, k):
        step = 1 if direction == 0 else -1
        source = a - step * h
        place = gg.at[rows_of(source), cols[k]]
        return remote(
            place, place, gs_sem.at[direction, h - 1], gr_sem.at[source, k],
            {"chip": c - step * B},
        )

    shared = PODS % 2 == 0
    mate = o + 1 - 2 * (o % 2)
    base, WN = (o % 2 * (N // 2), N // 2 // PIECES) if shared else (0, N // PIECES)
    w_copies, m_copies = [[] for _ in range(PIECES)], [[] for _ in range(PIECES)]
    for i in range(PIECES):
        piece = pl.ds(pl.multiple_of(base + i * WN, WN), WN)
        for d in range(1, B):
            here = wq.at[shard_of(b), piece]
            w_copies[i].append(remote(here, here, *family("w", i), member(0, d)))
            if shared:
                came = wq.at[shard_of((b - d + B) % B), piece]
                m_copies[i].append(remote(came, came, *family("m"), {"outer": mate}))
    rest = pl.ds(0, (B - 1) * S)
    w_part = [whole(wq.at[rest, pl.ds(0, WN)], "w", i) for i in range(PIECES)]
    w_all = whole(wq.at[rest, pl.ds(0, PIECES * WN)], "w")
    m_all = whole(wq.at[rest, pl.ds(0, PIECES * WN)], "m")

    def inward(direction):
        if direction == 0:
            return jnp.logical_and(a >= 1, a + 1 < A - 1)
        return jnp.logical_and(a <= A - 2, a - 1 >= 1)

    def g_first(k):
        for direction in range(2):
            @pl.when(g_sends(direction, 1))
            def _():
                g_copy(direction, 1, k).start()

    def g_out(k):
        for direction in range(2):
            @pl.when(jnp.logical_and(g_sends(direction, 1), jnp.logical_not(inward(direction))))
            def _():
                g_copy(direction, 1, k).start()

    def g_into(k):
        for direction in range(2):
            @pl.when(jnp.logical_and(g_sends(direction, 1), inward(direction)))
            def _():
                g_copy(direction, 1, k).start()

    ins[0].wait()
    start(c_copies)
    ins[1].wait()
    start(x_copies)
    ins[2].wait()
    for k in range(AHEAD):
        g_first(k)
    ins[3].wait()
    start(w_copies[0])
    for cp in ins[4:]:
        cp.wait()

    for k in range(K):
        high, low = halves(ev[:, cols[k]])
        eh[:, cols[k]] = high.astype(BF16)
        el[:, cols[k]] = low.astype(BF16)
    fed = thin_dot(bas[...], eh[...], el[...], 1)

    c_all.wait_recv()
    start(v_copies + b_copies[0])
    for copies in w_copies[1:]:
        start(copies)
    ball[0, :, :, share_of(o)] = bz[...]
    def y_copy(d, k):
        return remote(
            ysend.at[d - 1, :, cols[k]], yrecv.at[d - 1, :, cols[k]],
            *family("y"), member(0, d),
        )

    def gradient_chunk(k):
        for d in range(1, B):
            part = dot(xt[shard_of((b + d) % B), :], gg[:, cols[k]], 1, 0)
            ysend[d - 1, :, cols[k]] = part.astype(BF16)
            y_copy(d, k).start()
        ne_ref[:, cols[k]] = dot(xt[shard_of(b), :], gg[:, cols[k]], 1, 0)

    def y_in():
        y_all.wait_recv()

    def merge_chunk(k):
        part = ne_ref[:, cols[k]]
        for d in range(1, B):
            part = part + yrecv[d - 1, :, cols[k]].astype(F32)
        ne_ref[:, cols[k]] = part / TOK_DEV + ev[:, cols[k]]

    def o_copy(direction, r, k):
        s_buf, r_buf = (up_s, up_r) if direction == 0 else (dn_s, dn_r)
        return remote(
            s_buf.at[r - 1, :, cols[k]], r_buf.at[r - 1, :, cols[k]],
            rs_sem.at[direction, r - 1], rr_sem.at[a + r + 1 if direction == 0 else a - r, k],
            {"chip": c + B if direction == 0 else c - B},
        )

    def o_arrival(direction, r, k):
        r_buf = up_r if direction == 0 else dn_r
        place = r_buf.at[r - 1, :, cols[k]]
        return remote(
            place, place, rs_sem.at[direction, r - 1],
            rr_sem.at[a + r if direction == 0 else a + 1 - r, k],
            {"chip": c - B if direction == 0 else c + B},
        )

    def o_first(direction):
        return a == 0 if direction == 0 else a == A - 1

    def o_sends(direction, r):
        return a + r < A if direction == 0 else a - r >= 0

    def o_gets(direction, r):
        if direction == 0:
            return jnp.logical_and(a >= 1, a - 1 + r < A)
        return jnp.logical_and(a + 1 < A, a + 1 - r >= 0)

    def o_outer(direction):
        return a == A - 2 if direction == 0 else a == 1

    def out_piece(direction, r, k, first, outer=None):
        s_buf, r_buf = (up_s, up_r) if direction == 0 else (dn_s, dn_r)
        leads = o_first(direction)
        if not first:
            leads = jnp.logical_not(leads)
        if outer is not None:
            bound = o_outer(direction)
            leads = jnp.logical_and(leads, bound if outer else jnp.logical_not(bound))

        @pl.when(jnp.logical_and(o_sends(direction, r), leads))
        def _():
            token = a + r if direction == 0 else a - r
            part = dot(xg[rows_of(token), :], wq[:, cols[k]], 1, 0)
            if not first:
                o_arrival(direction, r + 1, k).wait_recv()
                part = part + r_buf[r, :, cols[k]].astype(F32)
            s_buf[r - 1, :, cols[k]] = part.astype(BF16)
            o_copy(direction, r, k).start()

    def basis_pass():
        v_all.wait_recv()
        for d in range(1, B):
            start(b_copies[d])

    def left_part():
        b_all.wait_recv()
        thin = jnp.zeros((B * A * R, T), F32)
        for k in range(K):
            basis = split(jnp.concatenate(
                [ball[d, t, :, cols[k]] for d in range(B) for t in range(A)], axis=0
            ))
            thin = thin + fold(dot(basis, gg[rows_of(a), cols[k]], 1, 1))
        for d in range(B):
            for t in range(A):
                row = (d * A + t) * R
                shard = shard_of(t * B + (b + d) % B)
                ls[t, d] = fold(dot(split(thin[row : row + R, :]), xv[:, shard], 1, 0)) / TOK_DEV
        start(j_copies)
        lz[a] = ls[a]


    def x_in():
        x_all.wait_recv()
        xt[...] = xg[...].T

    def weights_in():
        for came, passed in zip(w_part, m_copies):
            came.wait_recv()
            start(passed)

    def mates_in():
        if shared:
            m_all.wait_recv()

    def first_piece(r, k):
        for direction in range(2):
            out_piece(direction, r, k, True)

    def rest_piece(r, k):
        for direction in range(2):
            out_piece(direction, r, k, False)

    j_copies = along(lambda t: ls.at[t], lz.at[a], "j")
    def inner_piece(k):
        for direction in range(2):
            out_piece(direction, 1, k, False, False)

    def outer_piece(k):
        for direction in range(2):
            out_piece(direction, 1, k, False, True)

    l_copies = across(lambda do, db: left_s, lambda j, db: left_r.at[j], "l")
    z_copies = along(lambda t: zs.at[t], zr.at[a], "z")
    h_copies = across(
        lambda do, db: rp.at[db, :, :, share_of((o + do) % PODS)],
        lambda j, db: rq.at[j], "h",
    )
    t_copies = along(lambda t: rs.at[t], rw.at[a], "t")
    a_copies = along(lambda t: rz.at[a], rz.at[a], "a")
    p_copies = [
        remote(rz.at[a], rown.at[:, share_of(o)], *family("p"), member(do, 0))
        for do in range(1, PODS)
    ]
    f_copies = across(
        lambda do, db: rz, lambda j, db: rall.at[(-db) % B, :, :, share_of(o)], "f"
    )

    def left_line():
        j_all.wait_recv()
        for d in range(B):
            part = lz[0, d]
            for t in range(1, A):
                part = part + lz[t, d]
            left_s[d] = part + fed if d == 0 else part
        start(l_copies)

    left = []

    def left_done():
        total = [left_s[d] for d in range(B)]
        l_all.wait_recv()
        for j, (do, db) in enumerate(group):
            for d in range(B):
                total[d] = total[d] + left_r[j, (d + db) % B]
        left.extend(orthonormal(total[d] / PODS) for d in range(B))
        z = jnp.concatenate(
            [fold(dot(split(left[d]), xt[shard_of((b + d) % B), :], 1, 0)) for d in range(B)],
            axis=0,
        )
        for t in range(A):
            zs[t] = z[:, t * T : (t + 1) * T]
        start(z_copies)
        zr[a] = zs[a]

    z_wide = []

    def right_part():
        z_all.wait_recv()
        z_wide.append(split(jnp.concatenate(
            [zr[t, d * R : (d + 1) * R, :] for d in range(B) for t in range(A)], axis=0
        )))
        for k in range(K):
            part = fold(dot(z_wide[0], gg[rows_of(a), cols[k]], 1, 0)) / TOK_DEV
            lead = thin_dot(left[0], eh[:, cols[k]], el[:, cols[k]], 0)
            for d in range(B):
                for t in range(A):
                    row = (d * A + t) * R
                    piece = part[row : row + R]
                    if d == 0:
                        piece = piece + jnp.where(a == t, lead, 0.0)
                    rp[d, t, :, cols[k]] = piece.astype(BF16)
        start(h_copies)

    def right_group():
        right = rp[0, :, :, share_of(o)].astype(F32)
        h_all.wait_recv()
        for j in range(len(group)):
            right = right + rq[j].astype(F32)
        rs[...] = right.astype(BF16)
        start(t_copies)
        rw[a] = rs[a]

    def right_line():
        t_all.wait_recv()
        right = rw[0].astype(F32)
        for t in range(1, A):
            right = right + rw[t].astype(F32)
        rz[a] = (right / PODS).astype(BF16)
        start(a_copies + p_copies)
        rown[:, share_of(o)] = rz[a]

    def right_all():
        a_all.wait_recv()
        start(f_copies)
        rall[0, :, :, share_of(o)] = rz[...]

    def own_out():
        for k in range(K):
            own[:, cols[k]] = dot(xg[rows_of(a), :], wq[:, cols[k]], 1, 0)

    def hop(h, k):
        for direction in range(2):
            @pl.when(g_gets(direction, h))
            def _():
                g_arrival(direction, h, k).wait_recv()
            if h + 1 < A:
                @pl.when(g_sends(direction, h + 1))
                def _():
                    g_copy(direction, h + 1, k).start()

    def grad(k):
        gradient_chunk(k)

    actions = {
        "basis": basis_pass, "left0": left_part, "x": x_in, "out": g_out, "into": g_into, "hop": hop,
        "grad": grad, "weights": weights_in, "mates": mates_in, "left1": left_line,
        "left2": left_done, "right1": right_part, "right2": right_group,
        "right3": right_line, "right4": right_all, "own": own_out,
        "first": first_piece, "rest": rest_piece,
        "inner": inner_piece, "outer": outer_piece, "y": y_in, "merge": merge_chunk,
    }
    for kind, *args in plan_of(A, K):
        actions[kind](*args)

    p_all.wait_recv()
    lefts = split(left[0])
    for k in range(K):
        mine = rown[:, cols[k]].astype(F32)
        ne_ref[:, cols[k]] = ne_ref[:, cols[k]] - dot(lefts, stack(mine, mine), 0, 0)

    f_all.wait_recv()
    for k in range(K):
        rights = jnp.concatenate(
            [rall[d, t, :, cols[k]].astype(F32) for d in range(B) for t in range(A)], axis=0
        )
        delta = dot(z_wide[0], stack(rights, rights), 0, 0)
        own[:, cols[k]] = own[:, cols[k]] - LEARNING_RATE * delta
    for k in range(K):
        for direction in range(2):
            r_buf = up_r if direction == 0 else dn_r

            @pl.when(o_gets(direction, 1))
            def _():
                o_arrival(direction, 1, k).wait_recv()

            @pl.when(jnp.logical_not(o_gets(direction, 1)))
            def _():
                r_buf[0, :, cols[k]] = jnp.zeros((T, CN), BF16)
        both = up_r[0, :, cols[k]].astype(F32) + dn_r[0, :, cols[k]].astype(F32)
        out_ref[:, cols[k]] = (own[:, cols[k]] + both).astype(BF16)

    for cp in (
        x_all, c_all, v_all, b_all, w_all, j_all, l_all, z_all, h_all, t_all, p_all, a_all, f_all,
        y_all,
    ):
        cp.wait_send()
    if shared:
        m_all.wait_send()
    for direction in range(2):
        for h in range(1, A):
            step = 1 if direction == 0 else -1

            @pl.when(g_sends(direction, h))
            def _():
                place = gg.at[rows_of(a - step * (h - 1))]
                remote(
                    place, place, gs_sem.at[direction, h - 1], gr_sem.at[0, 0],
                    {"chip": c + step * B},
                ).wait_send()

            @pl.when(o_sends(direction, h))
            def _():
                place = (up_s if direction == 0 else dn_s).at[h - 1]
                remote(
                    place, place, rs_sem.at[direction, h - 1], rr_sem.at[0, 0],
                    {"chip": c + step * B},
                ).wait_send()


def store(out_vmem, ne_vmem, out_hbm, ne_hbm, sem):
    copies = [
        pltpu.make_async_copy(ne_vmem, ne_hbm, sem.at[0]),
        pltpu.make_async_copy(out_vmem, out_hbm, sem.at[1]),
    ]
    for cp in copies:
        cp.start()
    for cp in copies:
        cp.wait()


def shards(inputs, out_grads, weight, start_basis, error_buffer):
    PODS, NC = lax.axis_size("outer"), lax.axis_size("chip")
    A = 4 if NC % 4 == 0 else NC
    B = NC // A
    T, D = inputs.shape
    N = out_grads.shape[1]
    S = weight.shape[0]
    R = start_basis.shape[0]
    Q = B * S
    K = CHUNKS
    G = PODS * B
    dma = pltpu.SemaphoreType.DMA
    vmem = pl.BlockSpec(memory_space=pltpu.VMEM)
    hbm = pl.BlockSpec(memory_space=pltpu.HBM)
    outputs, new_error = pl.pallas_call(
        functools.partial(kernel, A, B, PODS),
        out_shape=(
            pltpu.VMEM((T, N), BF16),
            pltpu.VMEM((S, N), F32),
        ),
        in_specs=[hbm] * 5,
        out_specs=(vmem, vmem),
        scratch_shapes=[
            pltpu.VMEM((T, D), BF16),
            pltpu.VMEM((A * T, Q), BF16),
            pltpu.VMEM((Q, A * T), BF16),
            pltpu.VMEM((A * T, N), BF16),
            pltpu.VMEM((Q, N), BF16),
            pltpu.VMEM((R, N), F32),
            pltpu.VMEM((A, R, N // PODS), F32),
            pltpu.VMEM((B, A, R, N), F32),
            pltpu.VMEM((S, N), F32),
            pltpu.VMEM((S, N), BF16),
            pltpu.VMEM((S, N), BF16),
            pltpu.VMEM((B - 1, S, N), BF16),
            pltpu.VMEM((B - 1, S, N), BF16),
            pltpu.VMEM((A - 1, T, N), BF16),
            pltpu.VMEM((A - 1, T, N), BF16),
            pltpu.VMEM((A - 1, T, N), BF16),
            pltpu.VMEM((A - 1, T, N), BF16),
            pltpu.VMEM((A, B, R, S), F32),
            pltpu.VMEM((A, B, R, S), F32),
            pltpu.VMEM((B, R, S), F32),
            pltpu.VMEM((G - 1, B, R, S), F32),
            pltpu.VMEM((A, B * R, T), F32),
            pltpu.VMEM((A, B * R, T), F32),
            pltpu.VMEM((B, A, R, N), BF16),
            pltpu.VMEM((G - 1, A, R, N // PODS), BF16),
            pltpu.VMEM((A, R, N // PODS), BF16),
            pltpu.VMEM((A, R, N // PODS), BF16),
            pltpu.VMEM((A, R, N // PODS), BF16),
            pltpu.VMEM((R, N), BF16),
            pltpu.VMEM((B, A, R, N), BF16),
            pltpu.VMEM((T, N), F32),
            dma((7,)), dma((len(FAMILIES),)), dma((len(FAMILIES) + PIECES - 1,)),
            dma((2, A - 1)), dma((A, K)), dma((2, A - 1)), dma((A + 1, K)),
        ],
        compiler_params=pltpu.CompilerParams(
            collective_id=0, has_side_effects=True, vmem_limit_bytes=40 * 1024 * 1024
        ),
        name="step",
    )(*[
        pltpu.with_memory_space_constraint(t, pltpu.HBM)
        for t in (inputs, out_grads, weight, start_basis, error_buffer[0])
    ])
    hbm_out = pl.BlockSpec(memory_space=pltpu.HBM)
    outputs, new_error = pl.pallas_call(
        store,
        out_shape=(
            jax.ShapeDtypeStruct((T, N), BF16),
            jax.ShapeDtypeStruct((S, N), F32),
        ),
        in_specs=[vmem] * 2,
        out_specs=(hbm_out, hbm_out),
        scratch_shapes=[dma((2,))],
        compiler_params=pltpu.CompilerParams(vmem_limit_bytes=8 * 1024 * 1024),
        name="store",
    )(outputs, new_error)
    return outputs, new_error[None]


def solution(mesh):
    return jax.shard_map(
        shards,
        mesh=mesh,
        in_specs=(
            P(("outer", "chip"), None),
            P(("outer", "chip"), None),
            P("chip", None),
            P("chip", None),
            P("outer", "chip", None),
        ),
        out_specs=(P(("outer", "chip"), None), P("outer", "chip", None)),
        check_vma=False,
    )
```

```python
import functools

import jax
import jax.numpy as jnp
from jax import lax
from jax.experimental import pallas as pl
from jax.experimental.pallas import tpu as pltpu
from jax.sharding import PartitionSpec as P

TOK_DEV = 128
LEARNING_RATE = 0.2
CHUNKS = 8
AHEAD = 4
PIECES = 2
FAMILIES = "abcfhjklmptuvxyzw"
F32 = jnp.float32
BF16 = jnp.bfloat16


def dot(a, b, ca, cb):
    return lax.dot_general(
        a, b, (((ca,), (cb,)), ((), ())), preferred_element_type=F32
    )


def halves(v):
    high = v.astype(BF16).astype(F32)
    return high, v - high


def stack(*parts):
    return jnp.concatenate(parts, axis=0).astype(BF16)


def split(thin):
    return stack(*halves(thin))


def fold(both):
    n = both.shape[0] // 2
    return both[:n] + both[n:]


def thin_dot(thin, wide_high, wide_low, cb):
    n = thin.shape[0]
    both = split(thin)
    return fold(dot(both, wide_high, 1, cb)) + dot(both[:n], wide_low, 1, cb)


def orthonormal(v):
    count = v.shape[0]
    row = lax.broadcasted_iota(jnp.int32, (count, 1), 0)
    for k in range(count):
        pivot = v[k : k + 1, :]
        d = jnp.sum(v * pivot, axis=1, keepdims=True)
        norm = d[k : k + 1, :] + 1.0
        scale = jnp.where(row > k, d / norm, 0.0)
        unit = pivot / jnp.sqrt(norm)
        v = jnp.where(row == k, unit, v - scale * pivot)
    return v


PLAN = (
    ("basis",), ("hop", 1, 1), ("left0",), ("out", 1), ("hop", 1, 1), ("edge", 1), ("lefthop", 1),
    ("weights",), ("edge", 1), ("hop", 1, 1), ("into", 1), ("hop", 1, 1), ("into", 1), ("x",),
    ("mates",), ("hop", 2, 1), ("into", 1), ("lefthop", 2), ("out", 1), ("first", 1),
    ("hop", 2, 1), ("hop", 1, 1), ("first", 1), ("hop", 2, 1), ("first", 2), ("left1",),
    ("first", 2), ("out", 1), ("grad",), ("grad",), ("first", 1), ("rest", 1), ("hop", 2, 1),
    ("left2",), ("rest", 1), ("edge", 1), ("hop", 1, 1), ("out", 1), ("first", 1), ("grad",),
    ("into", 1), ("rest", 1), ("edge", 1), ("hop", 2, 1), ("first", 1), ("right1",), ("first", 2),
    ("hop", 1, 1), ("hop", 2, 1), ("outer", 1), ("rest", 1), ("first", 1), ("hop", 1, 1),
    ("outer", 1), ("rest", 1), ("grad",), ("right2",), ("rest", 1), ("first", 2), ("hop", 2, 1),
    ("first", 1), ("grad",), ("righthop", 1), ("rest", 2), ("first", 1), ("hop", 2, 1), ("grad",),
    ("first", 1), ("rest", 1), ("righthop", 2), ("outer", 1), ("grad",), ("own",), ("right3",),
    ("first", 1), ("outer", 1), ("first", 1), ("rest", 1), ("first", 1), ("outer", 1),
    ("rest", 3), ("grad",), ("first", 3), ("outer", 2), ("first", 1), ("right4",), ("rest", 1),
    ("outer", 1), ("rest", 2), ("y",), ("merge",),
)


def plan_of(A, K):
    out = [("out", k) for k in range(AHEAD, K)]
    into = [("into", k) for k in range(AHEAD, K)]
    edge = [("edge", k) for k in range(AHEAD, K)]
    hops = [[("hop", h, k) for k in range(K)] for h in range(1, A)]
    grads = list(range(K))
    firsts = [("first", r, k) for r in range(A - 1, 0, -1) for k in range(K)]
    rests = [("rest", r, k) for r in range(A - 2, 1, -1) for k in range(K)]
    rests += [("inner", k) for k in range(K)]
    outers = [("outer", k) for k in range(K)]
    merges = [("merge", k) for k in range(K)]
    queues = {"out": out, "into": into, "edge": edge, "first": firsts, "rest": rests, "outer": outers, "merge": merges}
    steps = []

    def take(queue, count):
        steps.extend(queue[:count])
        del queue[:count]

    def gradient():
        k = grads.pop(0)
        for h in range(1, A):
            take(hops[h - 1], K - len(hops[h - 1]) <= k and k + 1 - (K - len(hops[h - 1])))
        steps.append(("grad", k))

    for kind, *args in PLAN:
        if kind == "hop":
            h, count = args
            if h < A:
                take(hops[h - 1], count)
        elif kind == "grad":
            if grads:
                gradient()
        elif kind[-3:] == "hop":
            lines = range(1, A - 1) if args[0] == 0 else [args[0]]
            steps.extend((kind, i) for i in lines if i < A - 1)
        elif kind in queues:
            take(queues[kind], args[0] if args else len(queues[kind]))
        else:
            if kind == "y":
                take(out, K)
                take(into, K)
                take(edge, K)
                while grads:
                    gradient()
            steps.append((kind,))
    return steps


def kernel(
    A, B, PODS,
    x_hbm, g_hbm, w_hbm, basis_hbm, err_hbm,
    out_ref, ne_ref,
    xv, xg, xt, gg, wq, bas, bz, ball, ev, eh, el, ysend, yrecv, up_s, up_r, dn_s, dn_r,
    ls, l_sum, l_up, l_dn, left_s, left_r, zs, zr, rp, rq, rs, r_sum, r_up, r_dn, rz, rown, rall, own,
    in_sem, send_sem, recv_sem, gs_sem, gr_sem, rs_sem, rr_sem,
):
    o = lax.axis_index("outer")
    c = lax.axis_index("chip")
    a, b = c // B, c % B
    T = x_hbm.shape[0]
    S, N = w_hbm.shape
    Q = B * S
    R = basis_hbm.shape[0]
    K = CHUNKS
    CN = N // K
    NP = N // PODS
    cols = [pl.ds(k * CN, CN) for k in range(K)]

    def rows_of(s):
        return pl.ds(pl.multiple_of(s * T, T), T)

    def shard_of(s):
        return pl.ds(pl.multiple_of(s * S, S), S)

    def share_of(s):
        return pl.ds(pl.multiple_of(s * NP, NP), NP)

    ins = [
        pltpu.make_async_copy(src, dst, in_sem.at[i])
        for i, (src, dst) in enumerate([
            (basis_hbm.at[:, share_of(o)], bz.at[a]),
            (x_hbm, xv),
            (g_hbm, gg.at[rows_of(a)]),
            (w_hbm, wq.at[shard_of(b)]),
            (basis_hbm, bas),
            (x_hbm.at[:, pl.ds(pl.multiple_of(a * Q, Q), Q)], xg.at[rows_of(a)]),
            (err_hbm, ev),
        ])
    ]
    for cp in ins:
        cp.start()

    line = [((a + d) % A) * B + b for d in range(1, A)]
    group = [(do, db) for do in range(PODS) for db in range(B) if do or db]

    def member(do, db):
        return {"outer": (o + do) % PODS, "chip": a * B + (b + db) % B}

    def remote(src, dst, ss, rs, where):
        return pltpu.make_async_remote_copy(
            src_ref=src, dst_ref=dst, send_sem=ss, recv_sem=rs,
            device_id=where, device_id_type=pl.DeviceIdType.MESH,
        )

    barrier = pltpu.get_barrier_semaphore()
    for t in line:
        pl.semaphore_signal(
            barrier, inc=1, device_id={"chip": t}, device_id_type=pl.DeviceIdType.MESH
        )
    for do, db in group:
        pl.semaphore_signal(
            barrier, inc=1, device_id=member(do, db), device_id_type=pl.DeviceIdType.MESH
        )
    pl.semaphore_wait(barrier, len(line) + len(group))

    def family(name, step=0):
        i = FAMILIES.index(name)
        return send_sem.at[i], recv_sem.at[i + step]

    def along(src, dst, name):
        return [
            remote(src((a + d) % A), dst, *family(name), {"chip": ((a + d) % A) * B + b})
            for d in range(1, A)
        ]

    def across(src, dst, name):
        return [
            remote(src(do, db), dst(j, db), *family(name), member(do, db))
            for j, (do, db) in enumerate(group)
        ]

    def whole(ref, name, step=0):
        return remote(ref, ref, *family(name, step), {"outer": (o + 1) % PODS})

    def start(copies):
        for cp in copies:
            cp.start()

    lines = pl.ds(0, A - 1)
    others = pl.ds(0, (PODS - 1) * NP)
    x_all = whole(xg.at[pl.ds(0, (A - 1) * T)], "x")
    c_all = whole(bz.at[lines], "c")
    v_all = whole(ball.at[pl.ds(0, B - 1), :, :, pl.ds(0, NP)], "v")
    b_all = whole(ball.at[:, :, :, others], "b")
    l_all = whole(left_r, "l")
    z_all = whole(zs.at[lines], "z")
    h_all = whole(rq, "h")
    p_all = whole(rown.at[:, others], "p")
    a_all = whole(rz.at[lines], "a")
    f_all = whole(rq, "f")
    y_all = whole(ysend, "y")

    x_copies = along(
        lambda t: xv.at[:, pl.ds(pl.multiple_of(t * Q, Q), Q)], xg.at[rows_of(a)], "x"
    )
    c_copies = along(lambda t: bz.at[a], bz.at[a], "c")
    b_copies = [
        [
            remote(
                bz if d == 0 else ball.at[d, :, :, share_of(o)],
                ball.at[d, :, :, share_of(o)],
                *family("b"), member(do, 0),
            )
            for do in range(1, PODS)
        ]
        for d in range(B)
    ]
    v_copies = [
        remote(bz, ball.at[(-d) % B, :, :, share_of(o)], *family("v"), member(0, d))
        for d in range(1, B)
    ]

    def g_copy(direction, h, k):
        step = 1 if direction == 0 else -1
        source = a - step * (h - 1)
        place = gg.at[rows_of(source), cols[k]]
        return remote(
            place, place, gs_sem.at[direction, h - 1], gr_sem.at[source, k],
            {"chip": c + step * B},
        )

    def g_sends(direction, h):
        return (
            jnp.logical_and(a - (h - 1) >= 0, a + 1 < A)
            if direction == 0
            else jnp.logical_and(a + (h - 1) < A, a >= 1)
        )

    def g_gets(direction, h):
        return a - h >= 0 if direction == 0 else a + h < A

    def g_arrival(direction, h, k):
        step = 1 if direction == 0 else -1
        source = a - step * h
        place = gg.at[rows_of(source), cols[k]]
        return remote(
            place, place, gs_sem.at[direction, h - 1], gr_sem.at[source, k],
            {"chip": c - step * B},
        )

    shared = PODS % 2 == 0
    mate = o + 1 - 2 * (o % 2)
    base, WN = (o % 2 * (N // 2), N // 2 // PIECES) if shared else (0, N // PIECES)
    w_copies, m_copies = [[] for _ in range(PIECES)], [[] for _ in range(PIECES)]
    for i in range(PIECES):
        piece = pl.ds(pl.multiple_of(base + i * WN, WN), WN)
        for d in range(1, B):
            here = wq.at[shard_of(b), piece]
            w_copies[i].append(remote(here, here, *family("w", i), member(0, d)))
            if shared:
                came = wq.at[shard_of((b - d + B) % B), piece]
                m_copies[i].append(remote(came, came, *family("m"), {"outer": mate}))
    rest = pl.ds(0, (B - 1) * S)
    w_part = [whole(wq.at[rest, pl.ds(0, WN)], "w", i) for i in range(PIECES)]
    w_all = whole(wq.at[rest, pl.ds(0, PIECES * WN)], "w")
    m_all = whole(wq.at[rest, pl.ds(0, PIECES * WN)], "m")

    def inward(direction):
        if direction == 0:
            return jnp.logical_and(a >= 1, a + 1 < A - 1)
        return jnp.logical_and(a <= A - 2, a - 1 >= 1)

    def g_first(k):
        for direction in range(2):
            @pl.when(g_sends(direction, 1))
            def _():
                g_copy(direction, 1, k).start()

    def g_out(k):
        for direction in range(2):
            last = a == A - 2 if direction == 0 else a == 1

            @pl.when(jnp.logical_and(last, jnp.logical_and(a >= 1, a <= A - 2)))
            def _():
                g_copy(direction, 1, k).start()

    def g_edge(k):
        for direction in range(2):
            @pl.when(a == 0 if direction == 0 else a == A - 1)
            def _():
                g_copy(direction, 1, k).start()

    def g_into(k):
        for direction in range(2):
            @pl.when(jnp.logical_and(g_sends(direction, 1), inward(direction)))
            def _():
                g_copy(direction, 1, k).start()

    ins[0].wait()
    start(c_copies)
    ins[1].wait()
    start(x_copies)
    ins[2].wait()
    for k in range(AHEAD):
        g_first(k)
    ins[3].wait()
    start(w_copies[0])
    for cp in ins[4:]:
        cp.wait()

    for k in range(K):
        high, low = halves(ev[:, cols[k]])
        eh[:, cols[k]] = high.astype(BF16)
        el[:, cols[k]] = low.astype(BF16)
    fed = thin_dot(bas[...], eh[...], el[...], 1)

    c_all.wait_recv()
    start(v_copies + b_copies[0])
    for copies in w_copies[1:]:
        start(copies)
    ball[0, :, :, share_of(o)] = bz[...]
    def y_copy(d, k):
        return remote(
            ysend.at[d - 1, :, cols[k]], yrecv.at[d - 1, :, cols[k]],
            *family("y"), member(0, d),
        )

    def gradient_chunk(k):
        for d in range(1, B):
            part = dot(xt[shard_of((b + d) % B), :], gg[:, cols[k]], 1, 0)
            ysend[d - 1, :, cols[k]] = part.astype(BF16)
            y_copy(d, k).start()
        ne_ref[:, cols[k]] = dot(xt[shard_of(b), :], gg[:, cols[k]], 1, 0)

    def y_in():
        y_all.wait_recv()

    def merge_chunk(k):
        part = ne_ref[:, cols[k]]
        for d in range(1, B):
            part = part + yrecv[d - 1, :, cols[k]].astype(F32)
        ne_ref[:, cols[k]] = part / TOK_DEV + ev[:, cols[k]]

    def o_copy(direction, r, k):
        s_buf, r_buf = (up_s, up_r) if direction == 0 else (dn_s, dn_r)
        return remote(
            s_buf.at[r - 1, :, cols[k]], r_buf.at[r - 1, :, cols[k]],
            rs_sem.at[direction, r - 1], rr_sem.at[a + r + 1 if direction == 0 else a - r, k],
            {"chip": c + B if direction == 0 else c - B},
        )

    def o_arrival(direction, r, k):
        r_buf = up_r if direction == 0 else dn_r
        place = r_buf.at[r - 1, :, cols[k]]
        return remote(
            place, place, rs_sem.at[direction, r - 1],
            rr_sem.at[a + r if direction == 0 else a + 1 - r, k],
            {"chip": c - B if direction == 0 else c + B},
        )

    def o_first(direction):
        return a == 0 if direction == 0 else a == A - 1

    def o_sends(direction, r):
        return a + r < A if direction == 0 else a - r >= 0

    def o_gets(direction, r):
        if direction == 0:
            return jnp.logical_and(a >= 1, a - 1 + r < A)
        return jnp.logical_and(a + 1 < A, a + 1 - r >= 0)

    def o_outer(direction):
        return a == A - 2 if direction == 0 else a == 1

    def out_piece(direction, r, k, first, outer=None):
        s_buf, r_buf = (up_s, up_r) if direction == 0 else (dn_s, dn_r)
        leads = o_first(direction)
        if not first:
            leads = jnp.logical_not(leads)
        if outer is not None:
            bound = o_outer(direction)
            leads = jnp.logical_and(leads, bound if outer else jnp.logical_not(bound))

        @pl.when(jnp.logical_and(o_sends(direction, r), leads))
        def _():
            token = a + r if direction == 0 else a - r
            part = dot(xg[rows_of(token), :], wq[:, cols[k]], 1, 0)
            if not first:
                o_arrival(direction, r + 1, k).wait_recv()
                part = part + r_buf[r, :, cols[k]].astype(F32)
            s_buf[r - 1, :, cols[k]] = part.astype(BF16)
            o_copy(direction, r, k).start()

    def line_copy(hop, direction, src, dst, name):
        part = pl.ds(hop + 1, A - 1 - hop) if direction == 0 else pl.ds(0, A - 1 - hop)
        to = c + B if direction == 0 else c - B
        return remote(src.at[part], dst.at[part], *family(name), {"chip": to})

    def at_hop(hop, direction):
        return a == hop if direction == 0 else a == A - 1 - hop

    def line_hop(hop, own_part, sums, came, names):
        for direction in range(2):
            @pl.when(at_hop(hop, direction))
            def _():
                dst = came[direction]
                if hop == 0:
                    src = own_part
                else:
                    line_copy(hop - 1, direction, dst, dst, names[direction]).wait_recv()
                    src = sums.at[direction]
                    for t in range(hop + 1, A) if direction == 0 else range(A - 1 - hop):
                        total = own_part[t].astype(F32) + dst[t].astype(F32)
                        src[t] = total.astype(src.dtype)
                line_copy(hop, direction, src, dst, names[direction]).start()

    def line_end(came, names):
        for direction in range(2):
            @pl.when(at_hop(A - 1, direction))
            def _():
                dst = came[direction]
                line_copy(A - 2, direction, dst, dst, names[direction]).wait_recv()

    def left_hop(hop):
        line_hop(hop, ls, l_sum, (l_up, l_dn), "jk")

    def right_hop(hop):
        line_hop(hop, rs, r_sum, (r_up, r_dn), "tu")

    def basis_pass():
        v_all.wait_recv()
        for d in range(1, B):
            start(b_copies[d])

    def left_part():
        b_all.wait_recv()
        thin = jnp.zeros((B * A * R, T), F32)
        for k in range(K):
            basis = split(jnp.concatenate(
                [ball[d, t, :, cols[k]] for d in range(B) for t in range(A)], axis=0
            ))
            thin = thin + fold(dot(basis, gg[rows_of(a), cols[k]], 1, 1))
        for d in range(B):
            for t in range(A):
                row = (d * A + t) * R
                shard = shard_of(t * B + (b + d) % B)
                ls[t, d] = fold(dot(split(thin[row : row + R, :]), xv[:, shard], 1, 0)) / TOK_DEV
        line_hop(0, ls, l_sum, (l_up, l_dn), "jk")


    def x_in():
        x_all.wait_recv()
        xt[...] = xg[...].T

    def weights_in():
        for came, passed in zip(w_part, m_copies):
            came.wait_recv()
            start(passed)

    def mates_in():
        if shared:
            m_all.wait_recv()

    def first_piece(r, k):
        for direction in range(2):
            out_piece(direction, r, k, True)

    def rest_piece(r, k):
        for direction in range(2):
            out_piece(direction, r, k, False)

    def inner_piece(k):
        for direction in range(2):
            out_piece(direction, 1, k, False, False)

    def outer_piece(k):
        for direction in range(2):
            out_piece(direction, 1, k, False, True)

    l_copies = across(lambda do, db: left_s, lambda j, db: left_r.at[j], "l")
    z_copies = along(lambda t: zs.at[t], zr.at[a], "z")
    h_copies = across(
        lambda do, db: rp.at[db, :, :, share_of((o + do) % PODS)],
        lambda j, db: rq.at[j], "h",
    )
    a_copies = along(lambda t: rz.at[a], rz.at[a], "a")
    p_copies = [
        remote(rz.at[a], rown.at[:, share_of(o)], *family("p"), member(do, 0))
        for do in range(1, PODS)
    ]
    f_copies = across(
        lambda do, db: rz, lambda j, db: rall.at[(-db) % B, :, :, share_of(o)], "f"
    )

    def left_line():
        line_end((l_up, l_dn), "jk")
        for d in range(B):
            part = ls[a, d] + jnp.where(a > 0, l_up[a, d], 0.0)
            part = part + jnp.where(a < A - 1, l_dn[a, d], 0.0)
            left_s[d] = part + fed if d == 0 else part
        start(l_copies)

    left = []

    def left_done():
        total = [left_s[d] for d in range(B)]
        l_all.wait_recv()
        for j, (do, db) in enumerate(group):
            for d in range(B):
                total[d] = total[d] + left_r[j, (d + db) % B]
        left.extend(orthonormal(total[d] / PODS) for d in range(B))
        z = jnp.concatenate(
            [fold(dot(split(left[d]), xt[shard_of((b + d) % B), :], 1, 0)) for d in range(B)],
            axis=0,
        )
        for t in range(A):
            zs[t] = z[:, t * T : (t + 1) * T]
        start(z_copies)
        zr[a] = zs[a]

    z_wide = []

    def right_part():
        z_all.wait_recv()
        z_wide.append(split(jnp.concatenate(
            [zr[t, d * R : (d + 1) * R, :] for d in range(B) for t in range(A)], axis=0
        )))
        for k in range(K):
            part = fold(dot(z_wide[0], gg[rows_of(a), cols[k]], 1, 0)) / TOK_DEV
            lead = thin_dot(left[0], eh[:, cols[k]], el[:, cols[k]], 0)
            for d in range(B):
                for t in range(A):
                    row = (d * A + t) * R
                    piece = part[row : row + R]
                    if d == 0:
                        piece = piece + jnp.where(a == t, lead, 0.0)
                    rp[d, t, :, cols[k]] = piece.astype(BF16)
        start(h_copies)

    def right_group():
        right = rp[0, :, :, share_of(o)].astype(F32)
        h_all.wait_recv()
        for j in range(len(group)):
            right = right + rq[j].astype(F32)
        rs[...] = right.astype(BF16)
        line_hop(0, rs, r_sum, (r_up, r_dn), "tu")

    def right_line():
        line_end((r_up, r_dn), "tu")
        right = rs[a].astype(F32) + jnp.where(a > 0, r_up[a].astype(F32), 0.0)
        right = right + jnp.where(a < A - 1, r_dn[a].astype(F32), 0.0)
        rz[a] = (right / PODS).astype(BF16)
        start(a_copies + p_copies)
        rown[:, share_of(o)] = rz[a]

    def right_all():
        a_all.wait_recv()
        start(f_copies)
        rall[0, :, :, share_of(o)] = rz[...]

    def own_out():
        for k in range(K):
            own[:, cols[k]] = dot(xg[rows_of(a), :], wq[:, cols[k]], 1, 0)

    def hop(h, k):
        for direction in range(2):
            @pl.when(g_gets(direction, h))
            def _():
                g_arrival(direction, h, k).wait_recv()
            if h + 1 < A:
                @pl.when(g_sends(direction, h + 1))
                def _():
                    g_copy(direction, h + 1, k).start()

    def grad(k):
        gradient_chunk(k)

    actions = {
        "basis": basis_pass, "left0": left_part, "x": x_in, "out": g_out, "into": g_into,
        "edge": g_edge, "hop": hop,
        "grad": grad, "weights": weights_in, "mates": mates_in, "left1": left_line,
        "left2": left_done, "right1": right_part, "right2": right_group,
        "right3": right_line, "right4": right_all, "own": own_out,
        "first": first_piece, "rest": rest_piece,
        "inner": inner_piece, "outer": outer_piece, "y": y_in, "lefthop": left_hop, "righthop": right_hop,
        "merge": merge_chunk,
    }
    for kind, *args in plan_of(A, K):
        actions[kind](*args)

    p_all.wait_recv()
    lefts = split(left[0])
    for k in range(K):
        mine = rown[:, cols[k]].astype(F32)
        ne_ref[:, cols[k]] = ne_ref[:, cols[k]] - dot(lefts, stack(mine, mine), 0, 0)

    f_all.wait_recv()
    for k in range(K):
        rights = jnp.concatenate(
            [rall[d, t, :, cols[k]].astype(F32) for d in range(B) for t in range(A)], axis=0
        )
        delta = dot(z_wide[0], stack(rights, rights), 0, 0)
        own[:, cols[k]] = own[:, cols[k]] - LEARNING_RATE * delta
    for k in range(K):
        for direction in range(2):
            r_buf = up_r if direction == 0 else dn_r

            @pl.when(o_gets(direction, 1))
            def _():
                o_arrival(direction, 1, k).wait_recv()

            @pl.when(jnp.logical_not(o_gets(direction, 1)))
            def _():
                r_buf[0, :, cols[k]] = jnp.zeros((T, CN), BF16)
        both = up_r[0, :, cols[k]].astype(F32) + dn_r[0, :, cols[k]].astype(F32)
        out_ref[:, cols[k]] = (own[:, cols[k]] + both).astype(BF16)

    for cp in (
        x_all, c_all, v_all, b_all, w_all, l_all, z_all, h_all, p_all, a_all, f_all, y_all,
    ):
        cp.wait_send()
    if shared:
        m_all.wait_send()
    for hop_index in range(A - 1):
        for direction in range(2):
            @pl.when(at_hop(hop_index, direction))
            def _():
                for own_part, names in ((ls, "jk"), (rs, "tu")):
                    line_copy(
                        hop_index, direction, own_part, own_part, names[direction]
                    ).wait_send()
    for direction in range(2):
        for h in range(1, A):
            step = 1 if direction == 0 else -1

            @pl.when(g_sends(direction, h))
            def _():
                place = gg.at[rows_of(a - step * (h - 1))]
                remote(
                    place, place, gs_sem.at[direction, h - 1], gr_sem.at[0, 0],
                    {"chip": c + step * B},
                ).wait_send()

            @pl.when(o_sends(direction, h))
            def _():
                place = (up_s if direction == 0 else dn_s).at[h - 1]
                remote(
                    place, place, rs_sem.at[direction, h - 1], rr_sem.at[0, 0],
                    {"chip": c + step * B},
                ).wait_send()


def store(out_vmem, ne_vmem, out_hbm, ne_hbm, sem):
    copies = [
        pltpu.make_async_copy(ne_vmem, ne_hbm, sem.at[0]),
        pltpu.make_async_copy(out_vmem, out_hbm, sem.at[1]),
    ]
    for cp in copies:
        cp.start()
    for cp in copies:
        cp.wait()


def shards(inputs, out_grads, weight, start_basis, error_buffer):
    PODS, NC = lax.axis_size("outer"), lax.axis_size("chip")
    A = 4 if NC % 4 == 0 else NC
    B = NC // A
    T, D = inputs.shape
    N = out_grads.shape[1]
    S = weight.shape[0]
    R = start_basis.shape[0]
    Q = B * S
    K = CHUNKS
    G = PODS * B
    dma = pltpu.SemaphoreType.DMA
    vmem = pl.BlockSpec(memory_space=pltpu.VMEM)
    hbm = pl.BlockSpec(memory_space=pltpu.HBM)
    outputs, new_error = pl.pallas_call(
        functools.partial(kernel, A, B, PODS),
        out_shape=(
            pltpu.VMEM((T, N), BF16),
            pltpu.VMEM((S, N), F32),
        ),
        in_specs=[hbm] * 5,
        out_specs=(vmem, vmem),
        scratch_shapes=[
            pltpu.VMEM((T, D), BF16),
            pltpu.VMEM((A * T, Q), BF16),
            pltpu.VMEM((Q, A * T), BF16),
            pltpu.VMEM((A * T, N), BF16),
            pltpu.VMEM((Q, N), BF16),
            pltpu.VMEM((R, N), F32),
            pltpu.VMEM((A, R, N // PODS), F32),
            pltpu.VMEM((B, A, R, N), F32),
            pltpu.VMEM((S, N), F32),
            pltpu.VMEM((S, N), BF16),
            pltpu.VMEM((S, N), BF16),
            pltpu.VMEM((B - 1, S, N), BF16),
            pltpu.VMEM((B - 1, S, N), BF16),
            pltpu.VMEM((A - 1, T, N), BF16),
            pltpu.VMEM((A - 1, T, N), BF16),
            pltpu.VMEM((A - 1, T, N), BF16),
            pltpu.VMEM((A - 1, T, N), BF16),
            pltpu.VMEM((A, B, R, S), F32),
            pltpu.VMEM((2, A, B, R, S), F32),
            pltpu.VMEM((A, B, R, S), F32),
            pltpu.VMEM((A, B, R, S), F32),
            pltpu.VMEM((B, R, S), F32),
            pltpu.VMEM((G - 1, B, R, S), F32),
            pltpu.VMEM((A, B * R, T), F32),
            pltpu.VMEM((A, B * R, T), F32),
            pltpu.VMEM((B, A, R, N), BF16),
            pltpu.VMEM((G - 1, A, R, N // PODS), BF16),
            pltpu.VMEM((A, R, N // PODS), BF16),
            pltpu.VMEM((2, A, R, N // PODS), BF16),
            pltpu.VMEM((A, R, N // PODS), BF16),
            pltpu.VMEM((A, R, N // PODS), BF16),
            pltpu.VMEM((A, R, N // PODS), BF16),
            pltpu.VMEM((R, N), BF16),
            pltpu.VMEM((B, A, R, N), BF16),
            pltpu.VMEM((T, N), F32),
            dma((7,)), dma((len(FAMILIES),)), dma((len(FAMILIES) + PIECES - 1,)),
            dma((2, A - 1)), dma((A, K)), dma((2, A - 1)), dma((A + 1, K)),
        ],
        compiler_params=pltpu.CompilerParams(
            collective_id=0, has_side_effects=True, vmem_limit_bytes=40 * 1024 * 1024
        ),
        name="step",
    )(*[
        pltpu.with_memory_space_constraint(t, pltpu.HBM)
        for t in (inputs, out_grads, weight, start_basis, error_buffer[0])
    ])
    hbm_out = pl.BlockSpec(memory_space=pltpu.HBM)
    outputs, new_error = pl.pallas_call(
        store,
        out_shape=(
            jax.ShapeDtypeStruct((T, N), BF16),
            jax.ShapeDtypeStruct((S, N), F32),
        ),
        in_specs=[vmem] * 2,
        out_specs=(hbm_out, hbm_out),
        scratch_shapes=[dma((2,))],
        compiler_params=pltpu.CompilerParams(vmem_limit_bytes=8 * 1024 * 1024),
        name="store",
    )(outputs, new_error)
    return outputs, new_error[None]


def solution(mesh):
    return jax.shard_map(
        shards,
        mesh=mesh,
        in_specs=(
            P(("outer", "chip"), None),
            P(("outer", "chip"), None),
            P("chip", None),
            P("chip", None),
            P("outer", "chip", None),
        ),
        out_specs=(P(("outer", "chip"), None), P("outer", "chip", None)),
        check_vma=False,
    )
```
